768 devices in a mesh: gx: 96 (over y, x, z_lo), gy: 8 (over z_hi, core).
Axes of the slice: x: 4, y: 8, z: 12 (z_hi: 4, z_lo: 3; z = z_hi * 3 + z_lo), core: 2. Of those that a mesh axis runs over, the one named last changes fastest.
Arguments:
- phase_pops: float32 [15, 192, 16, 1024], P(None, 'gx', None, 'gy'), may hold values from 0 to 0.1
- flow_pops: float32 [19, 192, 16, 1024], P(None, 'gx', None, 'gy'), may hold values from 0 to 0.1
- solid_flags: int32 [192, 16, 1024], P('gx', None, 'gy'), may hold values 0 or 1
Outputs:
- phase_out: float32 [15, 192, 16, 1024], P(None, 'gx', None, 'gy')
- flow_out: float32 [19, 192, 16, 1024], P(None, 'gx', None, 'gy')
The draws below stay inside these ranges and needn't reach their ends.
All inputs are finite; a program needn't handle non-finite values. No bound on the sum of `solid_flags` on one device may be relied on, other than what follows from the above.
Results may differ from the reference program's by a relative error of at most 0.0001.
Values sent between devices are 32-bit elements; how exact they have to be, the bound alone decides.
No kernel may reach another device: no remote copies, remote signals or barrier semaphores. Data moves between devices by JAX's collectives and lax.ppermute only.
A program may use at most 32 MiB of HBM per device.

```python
import jax
import jax.numpy as jnp
from jax import lax

STEPS = 2
NX = 192
NY = 1024
NZ = 16


def set_ends(result, stream_key, smallest, largest):
    longest = result.shape.index(max(result.shape))
    spots = []
    for shift in (0, 1):
        where = [jax.random.randint(jax.random.fold_in(stream_key, axis), (), 0, length) for axis, length in enumerate(result.shape)]
        where[longest] = (where[longest] + shift) % result.shape[longest]
        spots.append(tuple(where))
    return result.at[spots[0]].set(smallest).at[spots[1]].set(largest)


def levels(rng, extent, pieces, low, top_value):
    def one(axis_at, blocks):
        draws = jax.random.uniform(jax.random.fold_in(jax.random.fold_in(rng, 6), axis_at), (blocks,), jnp.float32, low / len(pieces), top_value / len(pieces))
        return jnp.repeat(jnp.exp(draws), extent[axis_at] // blocks).reshape((-1,) + (1,) * (len(extent) - axis_at - 1))

    gain = one(*pieces[0])
    for cut in pieces[1:]:
        gain = gain * one(*cut)
    return gain


def setup_inputs(seed: int = 0) -> dict:
    arg_keys = jax.random.split(jax.random.key(seed), 4)
    return {
        "phase_pops": jnp.clip(0.1 * jax.random.uniform(arg_keys[0], (15, NX, NZ, NY), jnp.float32) ** levels(arg_keys[0], (15, NX, NZ, NY), ((1, 96), (3, 8)), -0.2, 0.2), 0.0, 0.1),
        "flow_pops": jnp.clip(0.1 * jax.random.uniform(arg_keys[1], (19, NX, NZ, NY), jnp.float32) ** levels(arg_keys[1], (19, NX, NZ, NY), ((1, 96), (3, 8)), -0.2, 0.2), 0.0, 0.1),
        "solid_flags": set_ends((jax.random.randint(arg_keys[2], (NX, NZ, NY), 0, 8) < 1).astype(jnp.int32), jax.random.fold_in(arg_keys[2], 1), 0, 1),
    }


PHASE_VELOCITIES = [(0, 0, 0), (1, 0, 0), (-1, 0, 0), (0, 1, 0), (0, -1, 0), (0, 0, 1), (0, 0, -1), (1, 1, 1), (1, 1, -1), (1, -1, 1), (1, -1, -1), (-1, 1, 1), (-1, 1, -1), (-1, -1, 1), (-1, -1, -1)]
PHASE_WEIGHTS = [2.0 / 9.0] + [1.0 / 9.0] * 6 + [1.0 / 72.0] * 8
FLOW_VELOCITIES = [(0, 0, 0), (1, 0, 0), (-1, 0, 0), (0, 1, 0), (0, -1, 0), (0, 0, 1), (0, 0, -1), (1, 1, 0), (1, -1, 0), (-1, 1, 0), (-1, -1, 0), (1, 0, 1), (1, 0, -1), (-1, 0, 1), (-1, 0, -1), (0, 1, 1), (0, 1, -1), (0, -1, 1), (0, -1, -1)]
FLOW_WEIGHTS = [1.0 / 3.0] + [1.0 / 18.0] * 6 + [1.0 / 36.0] * 12
SURFACE_TENSION = 0.05
INTERFACE_WIDTH = 4.0
GRADIENT_FLOOR = 0.1
PHASE_LAMBDA = 0.3
PHASE_RELAX = 0.8

def reverse_of(velocities):
    return [velocities.index((-vector[0], -vector[1], -vector[2])) for vector in velocities]

def relax(phase_read, flow_read, phase_field, neighbours, solid_cells):
    gradient = []
    for coordinate in range(3):
        total = jnp.zeros_like(phase_field)
        for number in range(19):
            if FLOW_VELOCITIES[number][coordinate] != 0:
                total = total + FLOW_WEIGHTS[number] * FLOW_VELOCITIES[number][coordinate] * neighbours[number]
        gradient.append(3.0 * total)
    laplacian = jnp.zeros_like(phase_field)
    for number in range(1, 19):
        laplacian = laplacian + FLOW_WEIGHTS[number] * (neighbours[number] - phase_field)
    laplacian = 6.0 * laplacian
    magnitude = jnp.sqrt(gradient[0] ** 2 + gradient[1] ** 2 + gradient[2] ** 2)
    scaling = 1.0 / jnp.maximum(magnitude, GRADIENT_FLOOR)
    normal = [component * scaling for component in gradient]
    clipped = jnp.clip(phase_field, 0.0, 1.0)
    density = 1.0 + 2.0 * clipped
    relax_time = 0.6 + 0.4 * clipped
    beta_value = 12.0 * SURFACE_TENSION / INTERFACE_WIDTH
    kappa_value = 1.5 * SURFACE_TENSION * INTERFACE_WIDTH
    potential = 4.0 * beta_value * phase_field * (phase_field - 1.0) * (phase_field - 0.5) - kappa_value * laplacian
    force_terms = [potential * component for component in gradient]
    pressure = lax.optimization_barrier(jnp.sum(flow_read, axis=0))
    velocity = []
    for coordinate in range(3):
        moment = 0.5 * force_terms[coordinate]
        for number in range(19):
            if FLOW_VELOCITIES[number][coordinate] != 0:
                moment = moment + FLOW_VELOCITIES[number][coordinate] * flow_read[number]
        velocity.append(moment / density)
    speed_sq = velocity[0] ** 2 + velocity[1] ** 2 + velocity[2] ** 2
    force_factor = 3.0 * (1.0 - 0.5 / relax_time) / density
    flow_reverse = reverse_of(FLOW_VELOCITIES)
    flow_post = []
    for number in range(19):
        vector = FLOW_VELOCITIES[number]
        weight = FLOW_WEIGHTS[number]
        along = vector[0] * velocity[0] + vector[1] * velocity[1] + vector[2] * velocity[2]
        along_force = vector[0] * force_terms[0] + vector[1] * force_terms[1] + vector[2] * force_terms[2]
        equilibrium = weight * (pressure + 3.0 * along + 4.5 * along * along - 1.5 * speed_sq)
        current = flow_read[number]
        post_value = current - (current - equilibrium) / relax_time + weight * force_factor * along_force
        flow_post.append(jnp.where(solid_cells, flow_read[flow_reverse[number]], post_value))
    phase_reverse = reverse_of(PHASE_VELOCITIES)
    interface = PHASE_LAMBDA * phase_field * (1.0 - phase_field)
    phase_post = []
    for number in range(15):
        vector = PHASE_VELOCITIES[number]
        weight = PHASE_WEIGHTS[number]
        along = vector[0] * velocity[0] + vector[1] * velocity[1] + vector[2] * velocity[2]
        along_normal = vector[0] * normal[0] + vector[1] * normal[1] + vector[2] * normal[2]
        equilibrium = weight * (phase_field * (1.0 + 3.0 * along) + interface * along_normal)
        current = phase_read[number]
        post_value = current - (current - equilibrium) / PHASE_RELAX
        phase_post.append(jnp.where(solid_cells, phase_read[phase_reverse[number]], post_value))
    return (jnp.stack(phase_post), jnp.stack(flow_post))

def roll_field(values, vector):
    return jnp.roll(values, (vector[0], vector[2], vector[1]), axis=(0, 1, 2))

def reference(phase_pops, flow_pops, solid_flags):
    solid_cells = solid_flags > 0
    for step in range(STEPS):
        phase_read = jnp.stack([roll_field(phase_pops[number], PHASE_VELOCITIES[number]) for number in range(15)])
        phase_field = lax.optimization_barrier(jnp.sum(phase_read, axis=0))
        flow_read = jnp.stack([roll_field(flow_pops[number], FLOW_VELOCITIES[number]) for number in range(19)])
        neighbours = [roll_field(phase_field, (-vector[0], -vector[1], -vector[2])) for vector in FLOW_VELOCITIES]
        phase_pops, flow_pops = relax(phase_read, flow_read, phase_field, neighbours, solid_cells)
    return (phase_pops, flow_pops)
```

```python
import functools

import jax
import jax.numpy as jnp
from jax import lax
from jax.experimental import pallas as pl
from jax.experimental.pallas import tpu as pltpu
from jax.sharding import PartitionSpec as P

HV = [
    (0, 0, 0),
    (1, 0, 0),
    (-1, 0, 0),
    (0, 1, 0),
    (0, -1, 0),
    (0, 0, 1),
    (0, 0, -1),
    (1, 1, 1),
    (1, 1, -1),
    (1, -1, 1),
    (1, -1, -1),
    (-1, 1, 1),
    (-1, 1, -1),
    (-1, -1, 1),
    (-1, -1, -1),
]
HW = [2.0 / 9.0] + [1.0 / 9.0] * 6 + [1.0 / 72.0] * 8
FV = [
    (0, 0, 0),
    (1, 0, 0),
    (-1, 0, 0),
    (0, 1, 0),
    (0, -1, 0),
    (0, 0, 1),
    (0, 0, -1),
    (1, 1, 0),
    (1, -1, 0),
    (-1, 1, 0),
    (-1, -1, 0),
    (1, 0, 1),
    (1, 0, -1),
    (-1, 0, 1),
    (-1, 0, -1),
    (0, 1, 1),
    (0, 1, -1),
    (0, -1, 1),
    (0, -1, -1),
]
FW = [1.0 / 3.0] + [1.0 / 18.0] * 6 + [1.0 / 36.0] * 12
NH, NF = len(HV), len(FV)
BETA = 12.0 * 0.05 / 4.0
KAPPA = 1.5 * 0.05 * 4.0
FLOOR = 0.1
LAMBDA = 0.3
INV_RELAX = 1.0 / 0.8


def neg(v):
    return (-v[0], -v[1], -v[2])


def pairs(velocities):
    return [
        (i, velocities.index(neg(v))) for i, v in enumerate(velocities) if v > neg(v)
    ]


HP, FP = pairs(HV), pairs(FV)
H_FORE = [i for i, v in enumerate(HV) if v[0] == 1]
H_BACK = [i for i, v in enumerate(HV) if v[0] == -1]
F_FORE = [i for i, v in enumerate(FV) if v[0] == 1]
F_BACK = [i for i, v in enumerate(FV) if v[0] == -1]
DEEP = 4
SLOTS = 128 // DEEP
ROWS = [("h", i, r) for i in range(NH) for r in range(2)] + [
    ("f", i, r) for i in range(NF) for r in range(2)
] + [("s", 0, r) for r in range(2)]
EDGE_TILES = -(-len(ROWS) // SLOTS)
SENT = len(H_FORE) + len(F_FORE) + 1
F32 = jnp.float32


def lanes():
    return lax.broadcasted_iota(jnp.int32, (16, 128), 1)


def yroll(tile, shift):
    return pltpu.roll(tile, shift % 128, axis=1)


def zroll(tile, shift):
    return pltpu.roll(tile, shift % 16, axis=0)


def odd(axis):
    return lax.rem(lax.axis_index(axis), 2) == 1


def total(terms):
    terms = list(terms)
    while len(terms) > 1:
        terms = [
            terms[k] + terms[k + 1] if k + 1 < len(terms) else terms[k]
            for k in range(0, len(terms), 2)
        ]
    return terms[0]


class Wide:
    def __init__(self, lane):
        self.first, self.last = lane == 0, lane == 127

    def shift(self, field, c, rim=True):
        if c == 0:
            return field
        edge = self.first if c == 1 else self.last
        own, out = yroll(field[0], c), yroll(field[1], c)
        return (
            jnp.where(edge, out, own),
            jnp.where(edge, own, out) if rim else None,
        )

    def pull(self, field, v, rim=True):
        if v[2]:
            field = (zroll(field[0], v[2]), zroll(field[1], v[2]))
        return self.shift(field, v[1], rim)


def add(a, b):
    return (a[0] + b[0], a[1] + b[1])


def edges_kernel(h_ref, f_ref, s_ref, a_ref, b_ref):
    lane = lanes()
    slot = lane // DEEP
    right = [jnp.zeros((16, 128), F32) for _ in range(EDGE_TILES)]
    left = [jnp.zeros((16, 128), F32) for _ in range(EDGE_TILES)]
    for k, (kind, i, r) in enumerate(ROWS):
        t, s = divmod(k, SLOTS)
        if kind == "s":
            source = (s_ref[r] > 0).astype(F32)
        else:
            source = h_ref[i, r] if kind == "h" else f_ref[i, r]
        turned = yroll(source, DEEP * (s + 1))
        right[t] = jnp.where(slot == s, turned, right[t])
        left[t] = jnp.where(slot == (s + 1) % SLOTS, turned, left[t])
    swap = odd("gy")
    for t in range(EDGE_TILES):
        left_tile = yroll(left[t], -DEEP)
        a_ref[t] = jnp.where(swap, left_tile, right[t])
        b_ref[t] = jnp.where(swap, right[t], left_tile)


def spread_edges(a_ref, b_ref):
    lane = lanes()
    even_slot = lax.rem(lane // DEEP, 2) == 0
    swap = odd("gy")
    mixed = []
    for t in range(EDGE_TILES):
        a, b = a_ref[t], b_ref[t]
        after = jnp.where(swap, b, a)
        before = yroll(jnp.where(swap, a, b), -DEEP)
        mixed.append(
            (jnp.where(even_slot, after, before), jnp.where(even_slot, before, after))
        )
    places = {row: k for k, row in enumerate(ROWS)}

    def rim(kind, i, r):
        t, s = divmod(places[(kind, i, r)], SLOTS)
        return yroll(mixed[t][s % 2], -DEEP * s)

    return rim


def stream(get_h, get_f, hs_ref, fs_ref, sums_ref, a_ref, b_ref, rim_of_f):
    lane = lanes()
    wide = Wide(lane)

    def put(ref, i, r, field):
        for t in range(ref.shape[2]):
            ref[i, r, t] = field[t]

    sent = {"fore": [], "back": []}
    part = {"fore": [], "back": []}
    for i, v in enumerate(HV):
        pulled = [wide.pull(get_h(i, r), v) for r in range(2)]
        if v[0] == 0:
            put(hs_ref, i, 0, pulled[0])
            put(hs_ref, i, 1, pulled[1])
            part["fore"].append(pulled[1])
            part["back"].append(pulled[0])
        elif v[0] == 1:
            put(hs_ref, i, 1, pulled[0])
            sent["fore"].append(pulled[1])
            part["fore"].append(pulled[0])
        else:
            put(hs_ref, i, 0, pulled[1])
            sent["back"].append(pulled[0])
            part["back"].append(pulled[1])
    for n, way in enumerate(("fore", "back")):
        kept = functools.reduce(add, sent[way])
        sums_ref[n, 0] = kept[0]
        sums_ref[n, 1] = kept[1]
    for i, v in enumerate(FV):
        pulled = [wide.pull(get_f(i, r), v, rim_of_f) for r in range(2)]
        if v[0] == 0:
            put(fs_ref, i, 0, pulled[0])
            put(fs_ref, i, 1, pulled[1])
        elif v[0] == 1:
            put(fs_ref, i, 1, pulled[0])
            sent["fore"].append(pulled[1])
        else:
            put(fs_ref, i, 0, pulled[1])
            sent["back"].append(pulled[0])
    swap = odd("gx")
    packed = []
    for way in ("fore", "back"):
        fields = sent[way] + [functools.reduce(add, part[way])]
        rims = jnp.zeros((16, 128), F32)
        for j, field in enumerate(fields):
            if field[1] is not None:
                rims = jnp.where(lane // 8 == j, yroll(field[1], 8 * j + 4), rims)
        packed.append([field[0] for field in fields] + [rims])
    for j in range(SENT + 1):
        a_ref[j] = jnp.where(swap, packed[1][j], packed[0][j])
        b_ref[j] = jnp.where(swap, packed[0][j], packed[1][j])


def collide(hs_ref, fs_ref, sums_ref, a_ref, b_ref, solid_of, new_h, new_f, scratch, tiles):
    got_ref, phi_ref, grad_ref = scratch
    lane = lanes()
    wide = Wide(lane)
    swap = odd("gx")
    rims = (
        jnp.where(swap, a_ref[SENT], b_ref[SENT]),
        jnp.where(swap, b_ref[SENT], a_ref[SENT]),
    )
    for j in range(SENT):
        a, b = a_ref[j], b_ref[j]
        got_ref[0, j, 0] = jnp.where(swap, a, b)
        got_ref[1, j, 0] = jnp.where(swap, b, a)
        for n in range(2):
            got_ref[n, j, 1] = yroll(rims[n], -(8 * j + 4))

    def h_at(i, r, t, zs):
        if r == 0 and HV[i][0] == 1:
            return got_ref[0, H_FORE.index(i), t, zs]
        if r == 1 and HV[i][0] == -1:
            return got_ref[1, H_BACK.index(i), t, zs]
        return hs_ref[i, r, t, zs]

    def f_at(i, r, t, zs):
        if r == 0 and FV[i][0] == 1:
            return got_ref[0, len(H_FORE) + F_FORE.index(i), t, zs]
        if r == 1 and FV[i][0] == -1:
            return got_ref[1, len(H_BACK) + F_BACK.index(i), t, zs]
        return fs_ref[i, r, t, zs]

    every = slice(None)
    for t in range(2):
        phi_ref[0, t] = got_ref[0, SENT - 1, t] + sums_ref[1, t]
        phi_ref[3, t] = got_ref[1, SENT - 1, t] + sums_ref[0, t]
        for r in range(2):
            phi_ref[r + 1, t] = total(h_at(i, r, t, every) for i in range(NH))
    for r in range(2):
        below, own, above = [(phi_ref[q, 0], phi_ref[q, 1]) for q in (r, r + 1, r + 2)]
        across = (above[0] - below[0], above[1] - below[1])
        around = add(above, below)
        upright = tuple(zroll(own[t], 1) + zroll(own[t], -1) for t in range(2))
        third = tuple(
            (1.0 / 3.0) * own[t] + (1.0 / 6.0) * (around[t] + upright[t]) for t in range(2)
        )
        rim = tiles == 2
        third_up, third_down = wide.shift(third, -1, rim), wide.shift(third, 1, rim)
        across_up, across_down = wide.shift(across, -1, rim), wide.shift(across, 1, rim)
        own_up, own_down = wide.shift(own, -1, rim), wide.shift(own, 1, rim)
        for t in range(tiles):
            along_y = own_up[t] + own_down[t]
            level = (1.0 / 6.0) * own[t] + (1.0 / 12.0) * (around[t] + along_y)
            grad_ref[r, t, 0] = (1.0 / 6.0) * across[t] + (1.0 / 12.0) * (
                across_up[t] + across_down[t] + zroll(across[t], 1) + zroll(across[t], -1)
            )
            grad_ref[r, t, 1] = 0.5 * (third_up[t] - third_down[t])
            grad_ref[r, t, 2] = zroll(level, -1) - zroll(level, 1)
            grad_ref[r, t, 3] = (
                (1.0 / 3.0) * (around[t] + upright[t])
                + (1.0 / 6.0) * (zroll(around[t], 1) + zroll(around[t], -1))
                + (third_up[t] + third_down[t])
                - 4.0 * own[t]
            )
    for r in range(2):
        for t in range(tiles):
            for z in (0, 8):
                zs = slice(z, z + 8)
                solid = solid_of(r, t, zs)
                phi = phi_ref[r + 1, t, zs]
                grad = [grad_ref[r, t, n, zs] for n in range(3)]
                collide_part(
                    phi,
                    grad,
                    grad_ref[r, t, 3, zs],
                    solid,
                    lambda i, r=r, t=t, zs=zs: h_at(i, r, t, zs),
                    lambda i, r=r, t=t, zs=zs: f_at(i, r, t, zs),
                    functools.partial(new_h, r, t, zs),
                    functools.partial(new_f, r, t, zs),
                )


def dot(v, u):
    terms = [(s, c) for s, c in zip(v, u, strict=True) if s]
    out = None
    for s, c in terms:
        if out is None:
            out = c if s > 0 else -c
        else:
            out = out + c if s > 0 else out - c
    return out


def collide_part(phi, grad, laplacian, solid, h_at, f_at, put_h, put_f):
    clipped = jnp.clip(phi, 0.0, 1.0)
    density = 1.0 + 2.0 * clipped
    relax = 0.6 + 0.4 * clipped
    inverse = 1.0 / (density * relax)
    rate, per_density = density * inverse, relax * inverse
    potential = (4.0 * BETA) * phi * (phi - 1.0) * (phi - 0.5) - KAPPA * laplacian
    force = [potential * g for g in grad]
    squared = grad[0] * grad[0] + grad[1] * grad[1] + grad[2] * grad[2]
    scale = 1.0 / jnp.maximum(jnp.sqrt(squared), FLOOR)
    f_rest = f_at(0)
    moment = [0.5 * c for c in force]
    pressure = f_rest
    for i, o in FP:
        fi, fo = f_at(i), f_at(o)
        difference = fi - fo
        pressure = pressure + (fi + fo)
        for n in range(3):
            if FV[i][n]:
                moment[n] = (
                    moment[n] + difference if FV[i][n] > 0 else moment[n] - difference
                )
    u = [m * per_density for m in moment]
    speed = u[0] * u[0] + u[1] * u[1] + u[2] * u[2]
    pull = 3.0 * (1.0 - 0.5 * rate) * per_density
    drive = [3.0 * rate * u[n] + pull * force[n] for n in range(3)]
    keep = 1.0 - rate
    level = rate * (pressure - 1.5 * speed)
    bend = 4.5 * rate
    put_f(0, jnp.where(solid, f_rest, keep * f_rest + FW[0] * level))
    for i, o in FP:
        w = FW[i]
        fi, fo = f_at(i), f_at(o)
        along = dot(FV[i], u)
        even = w * (level + bend * (along * along))
        uneven = w * dot(FV[i], drive)
        put_f(i, jnp.where(solid, fo, keep * fi + (even + uneven)))
        put_f(o, jnp.where(solid, fi, keep * fo + (even - uneven)))
    sharp = LAMBDA * phi * (1.0 - phi) * scale
    drift = [3.0 * phi * u[n] + sharp * grad[n] for n in range(3)]
    h_rest = h_at(0)
    stay = 1.0 - INV_RELAX
    put_h(0, jnp.where(solid, h_rest, stay * h_rest + (INV_RELAX * HW[0]) * phi))
    for i, o in HP:
        w = INV_RELAX * HW[i]
        hi, ho = h_at(i), h_at(o)
        even = w * phi
        uneven = w * dot(HV[i], drift)
        put_h(i, jnp.where(solid, ho, stay * hi + (even + uneven)))
        put_h(o, jnp.where(solid, hi, stay * ho + (even - uneven)))


def first_kernel(h_ref, f_ref, s_ref, ya_ref, yb_ref, a_ref, b_ref, hs_ref, fs_ref, sums_ref, so_ref):
    rim = spread_edges(ya_ref, yb_ref)
    for r in range(2):
        so_ref[r, 0] = (s_ref[r] > 0).astype(F32)
        so_ref[r, 1] = rim("s", 0, r)
    stream(
        lambda i, r: (h_ref[i, r], rim("h", i, r)),
        lambda i, r: (f_ref[i, r], rim("f", i, r)),
        hs_ref,
        fs_ref,
        sums_ref,
        a_ref,
        b_ref,
        True,
    )


def middle_kernel(
    hs_ref, fs_ref, sums_ref, s_ref, ra_ref, rb_ref,
    a_ref, b_ref, hs2_ref, fs2_ref, sums2_ref,
    h1_ref, f1_ref, got_ref, phi_ref, grad_ref,
):
    def new_h(r, t, zs, i, value):
        h1_ref[i, r, t, zs] = value

    def new_f(r, t, zs, i, value):
        f1_ref[i, r, t, zs] = value

    collide(
        hs_ref,
        fs_ref,
        sums_ref,
        ra_ref,
        rb_ref,
        lambda r, t, zs: s_ref[r, t, zs] > 0.5,
        new_h,
        new_f,
        (got_ref, phi_ref, grad_ref),
        2,
    )
    stream(
        lambda i, r: (h1_ref[i, r, 0], h1_ref[i, r, 1]),
        lambda i, r: (f1_ref[i, r, 0], f1_ref[i, r, 1]),
        hs2_ref,
        fs2_ref,
        sums2_ref,
        a_ref,
        b_ref,
        False,
    )


def last_kernel(
    hs_ref, fs_ref, sums_ref, s_ref, ra_ref, rb_ref,
    h_ref, f_ref,
    got_ref, phi_ref, grad_ref,
):
    def new_h(r, t, zs, i, value):
        h_ref[i, r, zs] = value

    def new_f(r, t, zs, i, value):
        f_ref[i, r, zs] = value

    collide(
        hs_ref,
        fs_ref,
        sums_ref,
        ra_ref,
        rb_ref,
        lambda r, t, zs: s_ref[r, t, zs] > 0.5,
        new_h,
        new_f,
        (got_ref, phi_ref, grad_ref),
        1,
    )


def call(kernel, outs, *args, scratch=()):
    spec = pl.BlockSpec(memory_space=pltpu.VMEM)
    return pl.pallas_call(
        kernel,
        out_shape=[jax.ShapeDtypeStruct(shape, F32) for shape in outs],
        in_specs=[spec] * len(args),
        out_specs=[spec] * len(outs),
        scratch_shapes=[pltpu.VMEM(shape, F32) for shape in scratch],
        compiler_params=pltpu.CompilerParams(vmem_limit_bytes=LIMIT),
    )(*args)


def swap_near(block, axis):
    return lax.ppermute(block, axis, [(i, i ^ 1) for i in range(lax.axis_size(axis))])


def swap_far(block, axis):
    n = lax.axis_size(axis)
    route = [(i, (i + 1) % n if i % 2 else (i - 1) % n) for i in range(n)]
    return lax.ppermute(block, axis, route)


TILE = (16, 128)
LIMIT = 16 * 1024 * 1024


def shards(phase_pops, flow_pops, solid_flags):
    edge, sent = (EDGE_TILES, *TILE), (SENT + 1, *TILE)
    a, b = call(edges_kernel, [edge, edge], phase_pops, flow_pops, solid_flags)
    a, b = swap_near(a, "gy"), swap_far(b, "gy")
    wide_h, wide_f = (NH, 2, 2, *TILE), (NF, 2, 2, *TILE)
    sums = (2, 2, *TILE)
    scratch = [(2, SENT, 2, *TILE), (4, 2, *TILE), (2, 2, 4, *TILE)]
    a, b, hs, fs, kept, solid = call(
        first_kernel,
        [sent, sent, wide_h, wide_f, sums, (2, 2, *TILE)],
        phase_pops,
        flow_pops,
        solid_flags,
        a,
        b,
    )
    a, b = swap_near(a, "gx"), swap_far(b, "gx")
    a, b, hs, fs, kept = call(
        middle_kernel,
        [sent, sent, wide_h, (NF, 2, 1, *TILE), sums],
        hs,
        fs,
        kept,
        solid,
        a,
        b,
        scratch=[wide_h, wide_f, *scratch],
    )
    a, b = swap_near(a, "gx"), swap_far(b, "gx")
    return tuple(
        call(
            last_kernel,
            [(NH, 2, *TILE), (NF, 2, *TILE)],
            hs,
            fs,
            kept,
            solid,
            a,
            b,
            scratch=scratch,
        )
    )


def solution(mesh):
    placed = (P(None, "gx", None, "gy"), P(None, "gx", None, "gy"), P("gx", None, "gy"))
    return jax.shard_map(
        shards,
        mesh=mesh,
        in_specs=placed,
        out_specs=placed[:2],
        check_vma=False,
    )
```

```python
import functools

import jax
import jax.numpy as jnp
from jax import lax
from jax.experimental import pallas as pl
from jax.experimental.pallas import tpu as pltpu
from jax.sharding import PartitionSpec as P

HV = [
    (0, 0, 0),
    (1, 0, 0),
    (-1, 0, 0),
    (0, 1, 0),
    (0, -1, 0),
    (0, 0, 1),
    (0, 0, -1),
    (1, 1, 1),
    (1, 1, -1),
    (1, -1, 1),
    (1, -1, -1),
    (-1, 1, 1),
    (-1, 1, -1),
    (-1, -1, 1),
    (-1, -1, -1),
]
HW = [2.0 / 9.0] + [1.0 / 9.0] * 6 + [1.0 / 72.0] * 8
FV = [
    (0, 0, 0),
    (1, 0, 0),
    (-1, 0, 0),
    (0, 1, 0),
    (0, -1, 0),
    (0, 0, 1),
    (0, 0, -1),
    (1, 1, 0),
    (1, -1, 0),
    (-1, 1, 0),
    (-1, -1, 0),
    (1, 0, 1),
    (1, 0, -1),
    (-1, 0, 1),
    (-1, 0, -1),
    (0, 1, 1),
    (0, 1, -1),
    (0, -1, 1),
    (0, -1, -1),
]
FW = [1.0 / 3.0] + [1.0 / 18.0] * 6 + [1.0 / 36.0] * 12
NH, NF = len(HV), len(FV)
BETA = 12.0 * 0.05 / 4.0
KAPPA = 1.5 * 0.05 * 4.0
FLOOR = 0.1
LAMBDA = 0.3
INV_RELAX = 1.0 / 0.8


def neg(v):
    return (-v[0], -v[1], -v[2])


def pairs(velocities):
    return [
        (i, velocities.index(neg(v))) for i, v in enumerate(velocities) if v > neg(v)
    ]


HP, FP = pairs(HV), pairs(FV)
H_FORE = [i for i, v in enumerate(HV) if v[0] == 1]
H_BACK = [i for i, v in enumerate(HV) if v[0] == -1]
F_FORE = [i for i, v in enumerate(FV) if v[0] == 1]
F_BACK = [i for i, v in enumerate(FV) if v[0] == -1]
DEEP = 4
SLOTS = 128 // DEEP
ROWS = [("h", i, r) for i in range(NH) for r in range(2)] + [
    ("f", i, r) for i in range(NF) for r in range(2)
] + [("s", 0, r) for r in range(2)]
EDGE_TILES = -(-len(ROWS) // SLOTS)
SENT = len(H_FORE) + len(F_FORE) + 1
F32 = jnp.float32


def lanes():
    return lax.broadcasted_iota(jnp.int32, (16, 128), 1)


def yroll(tile, shift):
    return pltpu.roll(tile, shift % 128, axis=1)


def zroll(tile, shift):
    return pltpu.roll(tile, shift % 16, axis=0)


def odd(axis):
    return lax.rem(lax.axis_index(axis), 2) == 1


def partner(ref, j, swap, near):
    if len(ref.shape) == 3:
        return ref[j]
    first, second = ref[0, j], ref[1, j]
    return jnp.where(swap, first, second) if near else jnp.where(swap, second, first)


def total(terms):
    terms = list(terms)
    while len(terms) > 1:
        terms = [
            terms[k] + terms[k + 1] if k + 1 < len(terms) else terms[k]
            for k in range(0, len(terms), 2)
        ]
    return terms[0]


def put(ref, i, r, field):
    for t in range(ref.shape[2]):
        ref[i, r, t] = field[t]


class Wide:
    def __init__(self, lane):
        self.first, self.last = lane == 0, lane == 127

    def shift(self, field, c, rim=True):
        if c == 0:
            return field
        edge = self.first if c == 1 else self.last
        own, out = yroll(field[0], c), yroll(field[1], c)
        return (
            jnp.where(edge, out, own),
            jnp.where(edge, own, out) if rim else None,
        )

    def pull(self, field, v, rim=True):
        if v[2]:
            field = (zroll(field[0], v[2]), zroll(field[1], v[2]))
        return self.shift(field, v[1], rim)


def add(a, b):
    return (a[0] + b[0], a[1] + b[1])


def slots_kernel(slot_ref):
    slot_ref[...] = lanes() // DEEP


def edges_kernel(slot_ref, h_ref, f_ref, s_ref, a_ref, b_ref):
    slot = slot_ref[...]
    right = [jnp.zeros((16, 128), F32) for _ in range(EDGE_TILES)]
    left = [jnp.zeros((16, 128), F32) for _ in range(EDGE_TILES)]
    for k, (kind, i, r) in enumerate(ROWS):
        t, s = divmod(k, SLOTS)
        if kind == "s":
            source = (s_ref[r] > 0).astype(F32)
        else:
            source = h_ref[i, r] if kind == "h" else f_ref[i, r]
        turned = yroll(source, DEEP * (s + 1))
        right[t] = jnp.where(slot == s, turned, right[t])
        left[t] = jnp.where(slot == (s + 1) % SLOTS, turned, left[t])
    swap = odd("gy")
    for t in range(EDGE_TILES):
        left_tile = yroll(left[t], -DEEP)
        a_ref[t] = jnp.where(swap, left_tile, right[t])
        b_ref[t] = jnp.where(swap, right[t], left_tile)


def spread_edges(a_ref, b_ref):
    lane = lanes()
    even_slot = lax.rem(lane // DEEP, 2) == 0
    swap = odd("gy")
    mixed = []
    for t in range(EDGE_TILES):
        a, b = partner(a_ref, t, swap, True), partner(b_ref, t, swap, False)
        after = jnp.where(swap, b, a)
        before = yroll(jnp.where(swap, a, b), -DEEP)
        mixed.append(
            (jnp.where(even_slot, after, before), jnp.where(even_slot, before, after))
        )
    places = {row: k for k, row in enumerate(ROWS)}

    def rim(kind, i, r):
        t, s = divmod(places[(kind, i, r)], SLOTS)
        return yroll(mixed[t][s % 2], -DEEP * s)

    return rim


def stream(get_h, get_f, hs_ref, sums_ref, a_ref, b_ref, rim_of_f):
    lane = lanes()
    wide = Wide(lane)
    sent = {"fore": [], "back": []}
    part = {"fore": [], "back": []}
    for i, v in enumerate(HV):
        pulled = [wide.pull(get_h(i, r), v) for r in range(2)]
        if v[0] == 0:
            put(hs_ref, i, 0, pulled[0])
            put(hs_ref, i, 1, pulled[1])
            part["fore"].append(pulled[1])
            part["back"].append(pulled[0])
        elif v[0] == 1:
            put(hs_ref, i, 1, pulled[0])
            sent["fore"].append(pulled[1])
            part["fore"].append(pulled[0])
        else:
            put(hs_ref, i, 0, pulled[1])
            sent["back"].append(pulled[0])
            part["back"].append(pulled[1])
    for n, way in enumerate(("fore", "back")):
        kept = functools.reduce(add, sent[way])
        sums_ref[n, 0] = kept[0]
        sums_ref[n, 1] = kept[1]
    for i in F_FORE:
        sent["fore"].append(wide.pull(get_f(i, 1), FV[i], rim_of_f))
    for i in F_BACK:
        sent["back"].append(wide.pull(get_f(i, 0), FV[i], rim_of_f))
    swap = odd("gx")
    packed = []
    for way in ("fore", "back"):
        fields = sent[way] + [functools.reduce(add, part[way])]
        rims = jnp.zeros((16, 128), F32)
        for j, field in enumerate(fields):
            if field[1] is not None:
                rims = jnp.where(lane // 8 == j, yroll(field[1], 8 * j + 4), rims)
        packed.append([field[0] for field in fields] + [rims])
    for j in range(SENT + 1):
        a_ref[j] = jnp.where(swap, packed[1][j], packed[0][j])
        b_ref[j] = jnp.where(swap, packed[0][j], packed[1][j])


def stream_rest(get_f, fs_ref):
    wide = Wide(lanes())
    for i, v in enumerate(FV):
        for r in range(2):
            if 0 <= r + v[0] < 2:
                put(fs_ref, i, r + v[0], wide.pull(get_f(i, r), v, fs_ref.shape[2] == 2))


def collide(hs_ref, fs_ref, sums_ref, a_ref, b_ref, solid_of, new_h, new_f, scratch, tiles, row_done=None):
    got_ref, phi_ref, grad_ref = scratch
    lane = lanes()
    wide = Wide(lane)
    swap = odd("gx")
    a, b = partner(a_ref, SENT, swap, True), partner(b_ref, SENT, swap, False)
    rims = jnp.where(swap, a, b), jnp.where(swap, b, a)
    for j in range(SENT):
        a, b = partner(a_ref, j, swap, True), partner(b_ref, j, swap, False)
        got_ref[0, j, 0] = jnp.where(swap, a, b)
        got_ref[1, j, 0] = jnp.where(swap, b, a)
        for n in range(2):
            got_ref[n, j, 1] = yroll(rims[n], -(8 * j + 4))

    def h_at(i, r, t, zs):
        if r == 0 and HV[i][0] == 1:
            return got_ref[0, H_FORE.index(i), t, zs]
        if r == 1 and HV[i][0] == -1:
            return got_ref[1, H_BACK.index(i), t, zs]
        return hs_ref[i, r, t, zs]

    def f_at(i, r, t, zs):
        if r == 0 and FV[i][0] == 1:
            return got_ref[0, len(H_FORE) + F_FORE.index(i), t, zs]
        if r == 1 and FV[i][0] == -1:
            return got_ref[1, len(H_BACK) + F_BACK.index(i), t, zs]
        return fs_ref[i, r, t, zs]

    every = slice(None)
    for t in range(2):
        phi_ref[0, t] = got_ref[0, SENT - 1, t] + sums_ref[1, t]
        phi_ref[3, t] = got_ref[1, SENT - 1, t] + sums_ref[0, t]
        for r in range(2):
            phi_ref[r + 1, t] = total(h_at(i, r, t, every) for i in range(NH))
    for r in range(2):
        below, own, above = [(phi_ref[q, 0], phi_ref[q, 1]) for q in (r, r + 1, r + 2)]
        across = (above[0] - below[0], above[1] - below[1])
        around = add(above, below)
        upright = tuple(zroll(own[t], 1) + zroll(own[t], -1) for t in range(2))
        third = tuple(
            (1.0 / 3.0) * own[t] + (1.0 / 6.0) * (around[t] + upright[t]) for t in range(2)
        )
        rim = tiles == 2
        third_up, third_down = wide.shift(third, -1, rim), wide.shift(third, 1, rim)
        across_up, across_down = wide.shift(across, -1, rim), wide.shift(across, 1, rim)
        own_up, own_down = wide.shift(own, -1, rim), wide.shift(own, 1, rim)
        for t in range(tiles):
            along_y = own_up[t] + own_down[t]
            level = (1.0 / 6.0) * own[t] + (1.0 / 12.0) * (around[t] + along_y)
            grad_ref[r, t, 0] = (1.0 / 6.0) * across[t] + (1.0 / 12.0) * (
                across_up[t] + across_down[t] + zroll(across[t], 1) + zroll(across[t], -1)
            )
            grad_ref[r, t, 1] = 0.5 * (third_up[t] - third_down[t])
            grad_ref[r, t, 2] = zroll(level, -1) - zroll(level, 1)
            grad_ref[r, t, 3] = (
                (1.0 / 3.0) * (around[t] + upright[t])
                + (1.0 / 6.0) * (zroll(around[t], 1) + zroll(around[t], -1))
                + (third_up[t] + third_down[t])
                - 4.0 * own[t]
            )
    for r in range(2):
        for t in range(tiles):
            for z in (0, 8):
                zs = slice(z, z + 8)
                solid = solid_of(r, t, zs)
                phi = phi_ref[r + 1, t, zs]
                grad = [grad_ref[r, t, n, zs] for n in range(3)]
                collide_part(
                    phi,
                    grad,
                    grad_ref[r, t, 3, zs],
                    solid,
                    lambda i, r=r, t=t, zs=zs: h_at(i, r, t, zs),
                    lambda i, r=r, t=t, zs=zs: f_at(i, r, t, zs),
                    functools.partial(new_h, r, t, zs),
                    functools.partial(new_f, r, t, zs),
                )
        if row_done is not None:
            row_done(r)


def dot(v, u):
    terms = [(s, c) for s, c in zip(v, u, strict=True) if s]
    out = None
    for s, c in terms:
        if out is None:
            out = c if s > 0 else -c
        else:
            out = out + c if s > 0 else out - c
    return out


def collide_part(phi, grad, laplacian, solid, h_at, f_at, put_h, put_f):
    clipped = jnp.clip(phi, 0.0, 1.0)
    density = 1.0 + 2.0 * clipped
    relax = 0.6 + 0.4 * clipped
    inverse = 1.0 / (density * relax)
    rate, per_density = density * inverse, relax * inverse
    potential = (4.0 * BETA) * phi * (phi - 1.0) * (phi - 0.5) - KAPPA * laplacian
    force = [potential * g for g in grad]
    squared = grad[0] * grad[0] + grad[1] * grad[1] + grad[2] * grad[2]
    scale = 1.0 / jnp.maximum(jnp.sqrt(squared), FLOOR)
    f_rest = f_at(0)
    moment = [0.5 * c for c in force]
    pressure = f_rest
    for i, o in FP:
        fi, fo = f_at(i), f_at(o)
        difference = fi - fo
        pressure = pressure + (fi + fo)
        for n in range(3):
            if FV[i][n]:
                moment[n] = (
                    moment[n] + difference if FV[i][n] > 0 else moment[n] - difference
                )
    u = [m * per_density for m in moment]
    speed = u[0] * u[0] + u[1] * u[1] + u[2] * u[2]
    pull = 3.0 * (1.0 - 0.5 * rate) * per_density
    drive = [3.0 * rate * u[n] + pull * force[n] for n in range(3)]
    keep = 1.0 - rate
    level = rate * (pressure - 1.5 * speed)
    bend = 4.5 * rate
    put_f(0, jnp.where(solid, f_rest, keep * f_rest + FW[0] * level))
    for i, o in FP:
        w = FW[i]
        fi, fo = f_at(i), f_at(o)
        along = dot(FV[i], u)
        even = w * (level + bend * (along * along))
        uneven = w * dot(FV[i], drive)
        put_f(i, jnp.where(solid, fo, keep * fi + (even + uneven)))
        put_f(o, jnp.where(solid, fi, keep * fo + (even - uneven)))
    sharp = LAMBDA * phi * (1.0 - phi) * scale
    drift = [3.0 * phi * u[n] + sharp * grad[n] for n in range(3)]
    h_rest = h_at(0)
    stay = 1.0 - INV_RELAX
    put_h(0, jnp.where(solid, h_rest, stay * h_rest + (INV_RELAX * HW[0]) * phi))
    for i, o in HP:
        w = INV_RELAX * HW[i]
        hi, ho = h_at(i), h_at(o)
        even = w * phi
        uneven = w * dot(HV[i], drift)
        put_h(i, jnp.where(solid, ho, stay * hi + (even + uneven)))
        put_h(o, jnp.where(solid, hi, stay * ho + (even - uneven)))


def first_kernel(h_ref, f_ref, s_ref, ya_ref, yb_ref, a_ref, b_ref, hs_ref, sums_ref, so_ref):
    rim = spread_edges(ya_ref, yb_ref)
    for r in range(2):
        so_ref[r, 0] = (s_ref[r] > 0).astype(F32)
        so_ref[r, 1] = rim("s", 0, r)
    stream(
        lambda i, r: (h_ref[i, r], rim("h", i, r)),
        lambda i, r: (f_ref[i, r], rim("f", i, r)),
        hs_ref,
        sums_ref,
        a_ref,
        b_ref,
        True,
    )


def first_rest_kernel(f_ref, ya_ref, yb_ref, fs_ref):
    rim = spread_edges(ya_ref, yb_ref)
    stream_rest(lambda i, r: (f_ref[i, r], rim("f", i, r)), fs_ref)


def middle_kernel(
    hs_ref, fs_ref, sums_ref, s_ref, ra_ref, rb_ref,
    a_ref, b_ref, hs2_ref, sums2_ref, f1_ref,
    h1_ref, got_ref, phi_ref, grad_ref,
):
    def new_h(r, t, zs, i, value):
        h1_ref[i, r, t, zs] = value

    def new_f(r, t, zs, i, value):
        f1_ref[i, r, t, zs] = value

    collide(
        hs_ref,
        fs_ref,
        sums_ref,
        ra_ref,
        rb_ref,
        lambda r, t, zs: s_ref[r, t, zs] > 0.5,
        new_h,
        new_f,
        (got_ref, phi_ref, grad_ref),
        2,
    )
    stream(
        lambda i, r: (h1_ref[i, r, 0], h1_ref[i, r, 1]),
        lambda i, r: (f1_ref[i, r, 0], f1_ref[i, r, 1]),
        hs2_ref,
        sums2_ref,
        a_ref,
        b_ref,
        False,
    )


def middle_rest_kernel(f1_ref, fs_ref):
    stream_rest(lambda i, r: (f1_ref[i, r, 0], f1_ref[i, r, 1]), fs_ref)


def last_kernel(
    hs_ref, fs_ref, sums_ref, s_ref, ra_ref, rb_ref,
    h_hbm, f_hbm,
    h_ref, f_ref, got_ref, phi_ref, grad_ref, sems,
):
    def new_h(r, t, zs, i, value):
        h_ref[r, i, zs] = value

    def new_f(r, t, zs, i, value):
        f_ref[r, i, zs] = value

    copies = []

    def row_done(r):
        for n, (source, target) in enumerate(((h_ref, h_hbm), (f_ref, f_hbm))):
            copies.append(
                pltpu.make_async_copy(source.at[r], target.at[:, r], sems.at[r, n])
            )
            copies[-1].start()

    collide(
        hs_ref,
        fs_ref,
        sums_ref,
        ra_ref,
        rb_ref,
        lambda r, t, zs: s_ref[r, t, zs] > 0.5,
        new_h,
        new_f,
        (got_ref, phi_ref, grad_ref),
        1,
        row_done,
    )
    for copy in copies:
        copy.wait()


HBM = pl.BlockSpec(memory_space=pltpu.HBM)
VMEM = pl.BlockSpec(memory_space=pltpu.VMEM)
TILE = (16, 128)
COVER = pl.CostEstimate(flops=2_000_000_000, bytes_accessed=4_000_000, transcendentals=0)
LIMIT = 16 * 1024 * 1024
NEAR_Y, FAR_Y, NEAR_X, FAR_X = True, False, True, False


def call(kernel, outs, *args, scratch=(), sems=None, source=VMEM, target=VMEM, cost=None):
    kept = [pltpu.VMEM(shape, F32) for shape in scratch]
    if sems is not None:
        kept.append(pltpu.SemaphoreType.DMA(sems))
    return pl.pallas_call(
        kernel,
        out_shape=[
            out if hasattr(out, "dtype") else jax.ShapeDtypeStruct(out, F32)
            for out in outs
        ],
        in_specs=[source] * len(args),
        out_specs=[target] * len(outs),
        scratch_shapes=kept,
        compiler_params=pltpu.CompilerParams(vmem_limit_bytes=LIMIT),
        cost_estimate=cost,
    )(*args)


def swap_near(block, axis, gather):
    n = lax.axis_size(axis)
    if gather:
        groups = [[i, i + 1] for i in range(0, n, 2)]
        return lax.all_gather(block, axis, axis_index_groups=groups)
    return lax.ppermute(block, axis, [(i, i ^ 1) for i in range(n)])


def swap_far(block, axis, gather):
    n = lax.axis_size(axis)
    if gather:
        groups = [[i, (i + 1) % n] for i in range(1, n, 2)]
        return lax.all_gather(block, axis, axis_index_groups=groups)
    route = [(i, (i + 1) % n if i % 2 else (i - 1) % n) for i in range(n)]
    return lax.ppermute(block, axis, route)


def shards(phase_pops, flow_pops, solid_flags):
    edge, sent = (EDGE_TILES, *TILE), (SENT + 1, *TILE)
    wide_h, wide_f = (NH, 2, 2, *TILE), (NF, 2, 2, *TILE)
    sums = (2, 2, *TILE)
    scratch = [(2, SENT, 2, *TILE), (4, 2, *TILE), (2, 2, 4, *TILE)]
    h, f = phase_pops, flow_pops
    (slot,) = call(slots_kernel, [jax.ShapeDtypeStruct(TILE, jnp.int32)], cost=COVER)
    a, b = call(edges_kernel, [edge, edge], slot, h, f, solid_flags)
    ya, yb = swap_near(a, "gy", NEAR_Y), swap_far(b, "gy", FAR_Y)
    a, b, hs, kept, solid = call(
        first_kernel, [sent, sent, wide_h, sums, (2, 2, *TILE)], h, f, solid_flags, ya, yb
    )
    a, b = swap_near(a, "gx", NEAR_X), swap_far(b, "gx", FAR_X)
    (fs,) = call(first_rest_kernel, [wide_f], f, ya, yb)
    a, b, hs, kept, f = call(
        middle_kernel,
        [sent, sent, wide_h, sums, wide_f],
        *(hs, fs, kept, solid, a, b),
        scratch=[wide_h, *scratch],
    )
    a, b = swap_near(a, "gx", NEAR_X), swap_far(b, "gx", FAR_X)
    (fs,) = call(middle_rest_kernel, [(NF, 2, 1, *TILE)], f)
    out_h, out_f = (NH, 2, *TILE), (NF, 2, *TILE)
    return tuple(
        call(
            last_kernel,
            [out_h, out_f],
            *(hs, fs, kept, solid, a, b),
            scratch=[(2, NH, *TILE), (2, NF, *TILE), *scratch],
            sems=(2, 2),
            target=HBM,
        )
    )


def solution(mesh):
    placed = (P(None, "gx", None, "gy"), P(None, "gx", None, "gy"), P("gx", None, "gy"))
    return jax.shard_map(
        shards,
        mesh=mesh,
        in_specs=placed,
        out_specs=placed[:2],
        check_vma=False,
    )
```

```python
import functools

import jax
import jax.numpy as jnp
from jax import lax
from jax.experimental import pallas as pl
from jax.experimental.pallas import tpu as pltpu
from jax.sharding import PartitionSpec as P

HV = [
    (0, 0, 0),
    (1, 0, 0),
    (-1, 0, 0),
    (0, 1, 0),
    (0, -1, 0),
    (0, 0, 1),
    (0, 0, -1),
    (1, 1, 1),
    (1, 1, -1),
    (1, -1, 1),
    (1, -1, -1),
    (-1, 1, 1),
    (-1, 1, -1),
    (-1, -1, 1),
    (-1, -1, -1),
]
HW = [2.0 / 9.0] + [1.0 / 9.0] * 6 + [1.0 / 72.0] * 8
FV = [
    (0, 0, 0),
    (1, 0, 0),
    (-1, 0, 0),
    (0, 1, 0),
    (0, -1, 0),
    (0, 0, 1),
    (0, 0, -1),
    (1, 1, 0),
    (1, -1, 0),
    (-1, 1, 0),
    (-1, -1, 0),
    (1, 0, 1),
    (1, 0, -1),
    (-1, 0, 1),
    (-1, 0, -1),
    (0, 1, 1),
    (0, 1, -1),
    (0, -1, 1),
    (0, -1, -1),
]
FW = [1.0 / 3.0] + [1.0 / 18.0] * 6 + [1.0 / 36.0] * 12
NH, NF = len(HV), len(FV)
BETA = 12.0 * 0.05 / 4.0
KAPPA = 1.5 * 0.05 * 4.0
FLOOR = 0.1
LAMBDA = 0.3
INV_RELAX = 1.0 / 0.8


def neg(v):
    return (-v[0], -v[1], -v[2])


def pairs(velocities):
    return [
        (i, velocities.index(neg(v))) for i, v in enumerate(velocities) if v > neg(v)
    ]


HP, FP = pairs(HV), pairs(FV)
H_FORE = [i for i, v in enumerate(HV) if v[0] == 1]
H_BACK = [i for i, v in enumerate(HV) if v[0] == -1]
F_FORE = [i for i, v in enumerate(FV) if v[0] == 1]
F_BACK = [i for i, v in enumerate(FV) if v[0] == -1]
DEEP = 4
SLOTS = 128 // DEEP
ROWS = [("h", i, r) for i in range(NH) for r in range(2)] + [
    ("f", i, r) for i in range(NF) for r in range(2)
] + [("s", 0, r) for r in range(2)]
EDGE_TILES = -(-len(ROWS) // SLOTS)
SENT = len(H_FORE) + len(F_FORE) + 1
F32 = jnp.float32


def lanes():
    return lax.broadcasted_iota(jnp.int32, (16, 128), 1)


def yroll(tile, shift):
    return pltpu.roll(tile, shift % 128, axis=1)


def zroll(tile, shift):
    return pltpu.roll(tile, shift % 16, axis=0)


def odd(axis):
    return lax.rem(lax.axis_index(axis), 2) == 1


def partner(ref, j, swap, near):
    if len(ref.shape) == 3:
        return ref[j]
    first, second = ref[0, j], ref[1, j]
    return jnp.where(swap, first, second) if near else jnp.where(swap, second, first)


def total(terms):
    terms = list(terms)
    while len(terms) > 1:
        terms = [
            terms[k] + terms[k + 1] if k + 1 < len(terms) else terms[k]
            for k in range(0, len(terms), 2)
        ]
    return terms[0]


def put(ref, i, r, field):
    for t in range(ref.shape[2]):
        ref[i, r, t] = field[t]


class Wide:
    def __init__(self, lane):
        self.first, self.last = lane == 0, lane == 127

    def shift(self, field, c, rim=True):
        if c == 0:
            return field
        edge = self.first if c == 1 else self.last
        own, out = yroll(field[0], c), yroll(field[1], c)
        return (
            jnp.where(edge, out, own),
            jnp.where(edge, own, out) if rim else None,
        )

    def pull(self, field, v, rim=True):
        if v[2]:
            field = (zroll(field[0], v[2]), zroll(field[1], v[2]))
        return self.shift(field, v[1], rim)


def add(a, b):
    return (a[0] + b[0], a[1] + b[1])


def slots_kernel(slot_ref):
    slot_ref[...] = lanes() // DEEP


def edges_kernel(slot_ref, h_ref, f_ref, s_ref, a_ref, b_ref):
    slot = slot_ref[...]
    right = [jnp.zeros((16, 128), F32) for _ in range(EDGE_TILES)]
    left = [jnp.zeros((16, 128), F32) for _ in range(EDGE_TILES)]
    for k, (kind, i, r) in enumerate(ROWS):
        t, s = divmod(k, SLOTS)
        if kind == "s":
            source = (s_ref[r] > 0).astype(F32)
        else:
            source = h_ref[i, r] if kind == "h" else f_ref[i, r]
        turned = yroll(source, DEEP * (s + 1))
        right[t] = jnp.where(slot == s, turned, right[t])
        left[t] = jnp.where(slot == (s + 1) % SLOTS, turned, left[t])
    swap = odd("gy")
    for t in range(EDGE_TILES):
        left_tile = yroll(left[t], -DEEP)
        a_ref[t] = jnp.where(swap, left_tile, right[t])
        b_ref[t] = jnp.where(swap, right[t], left_tile)


def spread_edges(a_ref, b_ref):
    lane = lanes()
    even_slot = lax.rem(lane // DEEP, 2) == 0
    swap = odd("gy")
    mixed = []
    for t in range(EDGE_TILES):
        a, b = partner(a_ref, t, swap, True), partner(b_ref, t, swap, False)
        after = jnp.where(swap, b, a)
        before = yroll(jnp.where(swap, a, b), -DEEP)
        mixed.append(
            (jnp.where(even_slot, after, before), jnp.where(even_slot, before, after))
        )
    places = {row: k for k, row in enumerate(ROWS)}

    def rim(kind, i, r):
        t, s = divmod(places[(kind, i, r)], SLOTS)
        return yroll(mixed[t][s % 2], -DEEP * s)

    return rim


def stream(get_h, get_f, hs_ref, sums_ref, a_ref, b_ref, rim_of_f):
    lane = lanes()
    wide = Wide(lane)
    sent = {"fore": [], "back": []}
    part = {"fore": [], "back": []}
    for i, v in enumerate(HV):
        pulled = [wide.pull(get_h(i, r), v) for r in range(2)]
        if v[0] == 0:
            put(hs_ref, i, 0, pulled[0])
            put(hs_ref, i, 1, pulled[1])
            part["fore"].append(pulled[1])
            part["back"].append(pulled[0])
        elif v[0] == 1:
            put(hs_ref, i, 1, pulled[0])
            sent["fore"].append(pulled[1])
            part["fore"].append(pulled[0])
        else:
            put(hs_ref, i, 0, pulled[1])
            sent["back"].append(pulled[0])
            part["back"].append(pulled[1])
    for n, way in enumerate(("fore", "back")):
        kept = functools.reduce(add, sent[way])
        sums_ref[n, 0] = kept[0]
        sums_ref[n, 1] = kept[1]
    for i in F_FORE:
        sent["fore"].append(wide.pull(get_f(i, 1), FV[i], rim_of_f))
    for i in F_BACK:
        sent["back"].append(wide.pull(get_f(i, 0), FV[i], rim_of_f))
    swap = odd("gx")
    packed = []
    for way in ("fore", "back"):
        fields = sent[way] + [functools.reduce(add, part[way])]
        rims = jnp.zeros((16, 128), F32)
        for j, field in enumerate(fields):
            if field[1] is not None:
                rims = jnp.where(lane // 8 == j, yroll(field[1], 8 * j + 4), rims)
        packed.append([field[0] for field in fields] + [rims])
    for j in range(SENT + 1):
        a_ref[j] = jnp.where(swap, packed[1][j], packed[0][j])
        b_ref[j] = jnp.where(swap, packed[0][j], packed[1][j])


def stream_rest(get_f, fs_ref):
    wide = Wide(lanes())
    for i, v in enumerate(FV):
        for r in range(2):
            if 0 <= r + v[0] < 2:
                put(fs_ref, i, r + v[0], wide.pull(get_f(i, r), v, fs_ref.shape[2] == 2))


def collide(hs_ref, fs_ref, sums_ref, a_ref, b_ref, solid_of, new_h, new_f, scratch, tiles, row_done=None):
    got_ref, phi_ref, grad_ref = scratch
    lane = lanes()
    wide = Wide(lane)
    swap = odd("gx")
    a, b = partner(a_ref, SENT, swap, True), partner(b_ref, SENT, swap, False)
    rims = jnp.where(swap, a, b), jnp.where(swap, b, a)
    for j in range(SENT):
        a, b = partner(a_ref, j, swap, True), partner(b_ref, j, swap, False)
        got_ref[0, j, 0] = jnp.where(swap, a, b)
        got_ref[1, j, 0] = jnp.where(swap, b, a)
        for n in range(2):
            got_ref[n, j, 1] = yroll(rims[n], -(8 * j + 4))

    def h_at(i, r, t, zs):
        if r == 0 and HV[i][0] == 1:
            return got_ref[0, H_FORE.index(i), t, zs]
        if r == 1 and HV[i][0] == -1:
            return got_ref[1, H_BACK.index(i), t, zs]
        return hs_ref[i, r, t, zs]

    def f_at(i, r, t, zs):
        if r == 0 and FV[i][0] == 1:
            return got_ref[0, len(H_FORE) + F_FORE.index(i), t, zs]
        if r == 1 and FV[i][0] == -1:
            return got_ref[1, len(H_BACK) + F_BACK.index(i), t, zs]
        return fs_ref[i, r, t, zs]

    every = slice(None)
    for t in range(2):
        phi_ref[0, t] = got_ref[0, SENT - 1, t] + sums_ref[1, t]
        phi_ref[3, t] = got_ref[1, SENT - 1, t] + sums_ref[0, t]
        for r in range(2):
            phi_ref[r + 1, t] = total(h_at(i, r, t, every) for i in range(NH))
    for r in range(2):
        below, own, above = [(phi_ref[q, 0], phi_ref[q, 1]) for q in (r, r + 1, r + 2)]
        across = (above[0] - below[0], above[1] - below[1])
        around = add(above, below)
        upright = tuple(zroll(own[t], 1) + zroll(own[t], -1) for t in range(2))
        third = tuple(
            (1.0 / 3.0) * own[t] + (1.0 / 6.0) * (around[t] + upright[t]) for t in range(2)
        )
        rim = tiles == 2
        third_up, third_down = wide.shift(third, -1, rim), wide.shift(third, 1, rim)
        across_up, across_down = wide.shift(across, -1, rim), wide.shift(across, 1, rim)
        own_up, own_down = wide.shift(own, -1, rim), wide.shift(own, 1, rim)
        for t in range(tiles):
            along_y = own_up[t] + own_down[t]
            level = (1.0 / 6.0) * own[t] + (1.0 / 12.0) * (around[t] + along_y)
            grad_ref[r, t, 0] = (1.0 / 6.0) * across[t] + (1.0 / 12.0) * (
                across_up[t] + across_down[t] + zroll(across[t], 1) + zroll(across[t], -1)
            )
            grad_ref[r, t, 1] = 0.5 * (third_up[t] - third_down[t])
            grad_ref[r, t, 2] = zroll(level, -1) - zroll(level, 1)
            grad_ref[r, t, 3] = (
                (1.0 / 3.0) * (around[t] + upright[t])
                + (1.0 / 6.0) * (zroll(around[t], 1) + zroll(around[t], -1))
                + (third_up[t] + third_down[t])
                - 4.0 * own[t]
            )
    for r in range(2):
        for t in range(tiles):
            for z in (0, 8):
                zs = slice(z, z + 8)
                solid = solid_of(r, t, zs)
                phi = phi_ref[r + 1, t, zs]
                grad = [grad_ref[r, t, n, zs] for n in range(3)]
                collide_part(
                    phi,
                    grad,
                    grad_ref[r, t, 3, zs],
                    solid,
                    lambda i, r=r, t=t, zs=zs: h_at(i, r, t, zs),
                    lambda i, r=r, t=t, zs=zs: f_at(i, r, t, zs),
                    functools.partial(new_h, r, t, zs),
                    functools.partial(new_f, r, t, zs),
                )
        if row_done is not None:
            row_done(r)


def dot(v, u):
    terms = [(s, c) for s, c in zip(v, u, strict=True) if s]
    out = None
    for s, c in terms:
        if out is None:
            out = c if s > 0 else -c
        else:
            out = out + c if s > 0 else out - c
    return out


def collide_part(phi, grad, laplacian, solid, h_at, f_at, put_h, put_f):
    clipped = jnp.clip(phi, 0.0, 1.0)
    density = 1.0 + 2.0 * clipped
    relax = 0.6 + 0.4 * clipped
    inverse = 1.0 / (density * relax)
    rate, per_density = density * inverse, relax * inverse
    potential = (4.0 * BETA) * phi * (phi - 1.0) * (phi - 0.5) - KAPPA * laplacian
    force = [potential * g for g in grad]
    squared = grad[0] * grad[0] + grad[1] * grad[1] + grad[2] * grad[2]
    scale = 1.0 / jnp.maximum(jnp.sqrt(squared), FLOOR)
    f_rest = f_at(0)
    moment = [0.5 * c for c in force]
    pressure = f_rest
    for i, o in FP:
        fi, fo = f_at(i), f_at(o)
        difference = fi - fo
        pressure = pressure + (fi + fo)
        for n in range(3):
            if FV[i][n]:
                moment[n] = (
                    moment[n] + difference if FV[i][n] > 0 else moment[n] - difference
                )
    u = [m * per_density for m in moment]
    speed = u[0] * u[0] + u[1] * u[1] + u[2] * u[2]
    pull = 3.0 * (1.0 - 0.5 * rate) * per_density
    drive = [3.0 * rate * u[n] + pull * force[n] for n in range(3)]
    keep = 1.0 - rate
    level = rate * (pressure - 1.5 * speed)
    bend = 4.5 * rate
    put_f(0, jnp.where(solid, f_rest, keep * f_rest + FW[0] * level))
    for i, o in FP:
        w = FW[i]
        fi, fo = f_at(i), f_at(o)
        along = dot(FV[i], u)
        even = w * (level + bend * (along * along))
        uneven = w * dot(FV[i], drive)
        put_f(i, jnp.where(solid, fo, keep * fi + (even + uneven)))
        put_f(o, jnp.where(solid, fi, keep * fo + (even - uneven)))
    sharp = LAMBDA * phi * (1.0 - phi) * scale
    drift = [3.0 * phi * u[n] + sharp * grad[n] for n in range(3)]
    h_rest = h_at(0)
    stay = 1.0 - INV_RELAX
    put_h(0, jnp.where(solid, h_rest, stay * h_rest + (INV_RELAX * HW[0]) * phi))
    for i, o in HP:
        w = INV_RELAX * HW[i]
        hi, ho = h_at(i), h_at(o)
        even = w * phi
        uneven = w * dot(HV[i], drift)
        put_h(i, jnp.where(solid, ho, stay * hi + (even + uneven)))
        put_h(o, jnp.where(solid, hi, stay * ho + (even - uneven)))


def first_kernel(h_ref, f_ref, s_ref, ya_ref, yb_ref, a_ref, b_ref, hs_ref, sums_ref, so_ref):
    rim = spread_edges(ya_ref, yb_ref)
    for r in range(2):
        so_ref[r, 0] = (s_ref[r] > 0).astype(F32)
        so_ref[r, 1] = rim("s", 0, r)
    stream(
        lambda i, r: (h_ref[i, r], rim("h", i, r)),
        lambda i, r: (f_ref[i, r], rim("f", i, r)),
        hs_ref,
        sums_ref,
        a_ref,
        b_ref,
        True,
    )


def first_rest_kernel(f_ref, ya_ref, yb_ref, fs_ref):
    rim = spread_edges(ya_ref, yb_ref)
    stream_rest(lambda i, r: (f_ref[i, r], rim("f", i, r)), fs_ref)


def middle_kernel(
    hs_ref, fs_ref, sums_ref, s_ref, ra_ref, rb_ref,
    a_ref, b_ref, hs2_ref, sums2_ref, f1_ref,
    h1_ref, got_ref, phi_ref, grad_ref,
):
    def new_h(r, t, zs, i, value):
        h1_ref[i, r, t, zs] = value

    def new_f(r, t, zs, i, value):
        f1_ref[i, r, t, zs] = value

    collide(
        hs_ref,
        fs_ref,
        sums_ref,
        ra_ref,
        rb_ref,
        lambda r, t, zs: s_ref[r, t, zs] > 0.5,
        new_h,
        new_f,
        (got_ref, phi_ref, grad_ref),
        2,
    )
    stream(
        lambda i, r: (h1_ref[i, r, 0], h1_ref[i, r, 1]),
        lambda i, r: (f1_ref[i, r, 0], f1_ref[i, r, 1]),
        hs2_ref,
        sums2_ref,
        a_ref,
        b_ref,
        False,
    )


def middle_rest_kernel(f1_ref, fs_ref):
    stream_rest(lambda i, r: (f1_ref[i, r, 0], f1_ref[i, r, 1]), fs_ref)


def last_kernel(
    hs_ref, fs_ref, sums_ref, s_ref, ra_ref, rb_ref,
    h_hbm, f_hbm,
    h_ref, f_ref, got_ref, phi_ref, grad_ref, sems,
):
    def new_h(r, t, zs, i, value):
        h_ref[r, i, zs] = value

    def new_f(r, t, zs, i, value):
        f_ref[r, i, zs] = value

    copies = []

    def row_done(r):
        for n, (source, target) in enumerate(((h_ref, h_hbm), (f_ref, f_hbm))):
            copies.append(
                pltpu.make_async_copy(source.at[r], target.at[:, r], sems.at[r, n])
            )
            copies[-1].start()

    collide(
        hs_ref,
        fs_ref,
        sums_ref,
        ra_ref,
        rb_ref,
        lambda r, t, zs: s_ref[r, t, zs] > 0.5,
        new_h,
        new_f,
        (got_ref, phi_ref, grad_ref),
        1,
        row_done,
    )
    for copy in copies:
        copy.wait()


HBM = pl.BlockSpec(memory_space=pltpu.HBM)
VMEM = pl.BlockSpec(memory_space=pltpu.VMEM)
TILE = (16, 128)
COVER = pl.CostEstimate(flops=2_000_000_000, bytes_accessed=4_000_000, transcendentals=0)
LIMIT = 16 * 1024 * 1024
NEAR_Y, FAR_Y, NEAR_X, FAR_X = True, True, True, False


def call(kernel, outs, *args, scratch=(), sems=None, source=VMEM, target=VMEM, cost=None):
    kept = [pltpu.VMEM(shape, F32) for shape in scratch]
    if sems is not None:
        kept.append(pltpu.SemaphoreType.DMA(sems))
    return pl.pallas_call(
        kernel,
        out_shape=[
            out if hasattr(out, "dtype") else jax.ShapeDtypeStruct(out, F32)
            for out in outs
        ],
        in_specs=[source] * len(args),
        out_specs=[target] * len(outs),
        scratch_shapes=kept,
        compiler_params=pltpu.CompilerParams(vmem_limit_bytes=LIMIT),
        cost_estimate=cost,
    )(*args)


def swap_near(block, axis, gather):
    n = lax.axis_size(axis)
    if gather:
        groups = [[i, i + 1] for i in range(0, n, 2)]
        return lax.all_gather(block, axis, axis_index_groups=groups)
    return lax.ppermute(block, axis, [(i, i ^ 1) for i in range(n)])


def swap_far(block, axis, gather):
    n = lax.axis_size(axis)
    if gather:
        groups = [[i, (i + 1) % n] for i in range(1, n, 2)]
        return lax.all_gather(block, axis, axis_index_groups=groups)
    route = [(i, (i + 1) % n if i % 2 else (i - 1) % n) for i in range(n)]
    return lax.ppermute(block, axis, route)


def shards(phase_pops, flow_pops, solid_flags):
    edge, sent = (EDGE_TILES, *TILE), (SENT + 1, *TILE)
    wide_h, wide_f = (NH, 2, 2, *TILE), (NF, 2, 2, *TILE)
    sums = (2, 2, *TILE)
    scratch = [(2, SENT, 2, *TILE), (4, 2, *TILE), (2, 2, 4, *TILE)]
    h, f = phase_pops, flow_pops
    (slot,) = call(slots_kernel, [jax.ShapeDtypeStruct(TILE, jnp.int32)], cost=COVER)
    a, b = call(edges_kernel, [edge, edge], slot, h, f, solid_flags)
    ya, yb = swap_near(a, "gy", NEAR_Y), swap_far(b, "gy", FAR_Y)
    a, b, hs, kept, solid = call(
        first_kernel, [sent, sent, wide_h, sums, (2, 2, *TILE)], h, f, solid_flags, ya, yb
    )
    a, b = swap_near(a, "gx", NEAR_X), swap_far(b, "gx", FAR_X)
    (fs,) = call(first_rest_kernel, [wide_f], f, ya, yb)
    a, b, hs, kept, f = call(
        middle_kernel,
        [sent, sent, wide_h, sums, wide_f],
        *(hs, fs, kept, solid, a, b),
        scratch=[wide_h, *scratch],
    )
    a, b = swap_near(a, "gx", NEAR_X), swap_far(b, "gx", FAR_X)
    (fs,) = call(middle_rest_kernel, [(NF, 2, 1, *TILE)], f)
    out_h, out_f = (NH, 2, *TILE), (NF, 2, *TILE)
    return tuple(
        call(
            last_kernel,
            [out_h, out_f],
            *(hs, fs, kept, solid, a, b),
            scratch=[(2, NH, *TILE), (2, NF, *TILE), *scratch],
            sems=(2, 2),
            target=HBM,
        )
    )


def solution(mesh):
    placed = (P(None, "gx", None, "gy"), P(None, "gx", None, "gy"), P("gx", None, "gy"))
    return jax.shard_map(
        shards,
        mesh=mesh,
        in_specs=placed,
        out_specs=placed[:2],
        check_vma=False,
    )
```

```python
import functools

import jax
import jax.numpy as jnp
from jax import lax
from jax.experimental import pallas as pl
from jax.experimental.pallas import tpu as pltpu
from jax.sharding import PartitionSpec as P

HV = [
    (0, 0, 0),
    (1, 0, 0),
    (-1, 0, 0),
    (0, 1, 0),
    (0, -1, 0),
    (0, 0, 1),
    (0, 0, -1),
    (1, 1, 1),
    (1, 1, -1),
    (1, -1, 1),
    (1, -1, -1),
    (-1, 1, 1),
    (-1, 1, -1),
    (-1, -1, 1),
    (-1, -1, -1),
]
HW = [2.0 / 9.0] + [1.0 / 9.0] * 6 + [1.0 / 72.0] * 8
FV = [
    (0, 0, 0),
    (1, 0, 0),
    (-1, 0, 0),
    (0, 1, 0),
    (0, -1, 0),
    (0, 0, 1),
    (0, 0, -1),
    (1, 1, 0),
    (1, -1, 0),
    (-1, 1, 0),
    (-1, -1, 0),
    (1, 0, 1),
    (1, 0, -1),
    (-1, 0, 1),
    (-1, 0, -1),
    (0, 1, 1),
    (0, 1, -1),
    (0, -1, 1),
    (0, -1, -1),
]
FW = [1.0 / 3.0] + [1.0 / 18.0] * 6 + [1.0 / 36.0] * 12
NH, NF = len(HV), len(FV)
BETA = 12.0 * 0.05 / 4.0
KAPPA = 1.5 * 0.05 * 4.0
FLOOR = 0.1
LAMBDA = 0.3
INV_RELAX = 1.0 / 0.8


def neg(v):
    return (-v[0], -v[1], -v[2])


def pairs(velocities):
    return [
        (i, velocities.index(neg(v))) for i, v in enumerate(velocities) if v > neg(v)
    ]


HP, FP = pairs(HV), pairs(FV)
H_FORE = [i for i, v in enumerate(HV) if v[0] == 1]
H_BACK = [i for i, v in enumerate(HV) if v[0] == -1]
F_FORE = [i for i, v in enumerate(FV) if v[0] == 1]
F_BACK = [i for i, v in enumerate(FV) if v[0] == -1]
DEEP = 4
SLOTS = 128 // DEEP
ROWS = [("h", i, r) for i in range(NH) for r in range(2)] + [
    ("f", i, r) for i in range(NF) for r in range(2)
] + [("s", 0, r) for r in range(2)]
EDGE_TILES = -(-len(ROWS) // SLOTS)
SENT = len(H_FORE) + len(F_FORE) + 1
F32 = jnp.float32


def lanes():
    return lax.broadcasted_iota(jnp.int32, (16, 128), 1)


def yroll(tile, shift):
    return pltpu.roll(tile, shift % 128, axis=1)


def zroll(tile, shift):
    return pltpu.roll(tile, shift % 16, axis=0)


def odd(axis):
    return lax.rem(lax.axis_index(axis), 2) == 1


def partner(ref, j, swap, near):
    if len(ref.shape) == 3:
        return ref[j]
    first, second = ref[0, j], ref[1, j]
    return jnp.where(swap, first, second) if near else jnp.where(swap, second, first)


def total(terms):
    terms = list(terms)
    while len(terms) > 1:
        terms = [
            terms[k] + terms[k + 1] if k + 1 < len(terms) else terms[k]
            for k in range(0, len(terms), 2)
        ]
    return terms[0]


def put(ref, i, r, field):
    for t in range(ref.shape[2]):
        ref[i, r, t] = field[t]


class Wide:
    def __init__(self, lane):
        self.first, self.last = lane == 0, lane == 127

    def shift(self, field, c, rim=True):
        if c == 0:
            return field
        edge = self.first if c == 1 else self.last
        own, out = yroll(field[0], c), yroll(field[1], c)
        return (
            jnp.where(edge, out, own),
            jnp.where(edge, own, out) if rim else None,
        )

    def pull(self, field, v, rim=True):
        if v[2]:
            field = (zroll(field[0], v[2]), zroll(field[1], v[2]))
        return self.shift(field, v[1], rim)


def add(a, b):
    return (a[0] + b[0], a[1] + b[1])


def slots_kernel(slot_ref):
    slot_ref[...] = lanes() // DEEP


def edges_kernel(slot_ref, h_ref, f_ref, s_ref, a_ref, b_ref):
    slot = slot_ref[...]
    right = [jnp.zeros((16, 128), F32) for _ in range(EDGE_TILES)]
    left = [jnp.zeros((16, 128), F32) for _ in range(EDGE_TILES)]
    for k, (kind, i, r) in enumerate(ROWS):
        t, s = divmod(k, SLOTS)
        if kind == "s":
            source = (s_ref[r] > 0).astype(F32)
        else:
            source = h_ref[i, r] if kind == "h" else f_ref[i, r]
        turned = yroll(source, DEEP * (s + 1))
        right[t] = jnp.where(slot == s, turned, right[t])
        left[t] = jnp.where(slot == (s + 1) % SLOTS, turned, left[t])
    swap = odd("gy")
    for t in range(EDGE_TILES):
        left_tile = yroll(left[t], -DEEP)
        a_ref[t] = jnp.where(swap, left_tile, right[t])
        b_ref[t] = jnp.where(swap, right[t], left_tile)


def spread_edges(a_ref, b_ref):
    lane = lanes()
    even_slot = lax.rem(lane // DEEP, 2) == 0
    swap = odd("gy")
    mixed = []
    for t in range(EDGE_TILES):
        a, b = partner(a_ref, t, swap, True), partner(b_ref, t, swap, False)
        after = jnp.where(swap, b, a)
        before = yroll(jnp.where(swap, a, b), -DEEP)
        mixed.append(
            (jnp.where(even_slot, after, before), jnp.where(even_slot, before, after))
        )
    places = {row: k for k, row in enumerate(ROWS)}

    def rim(kind, i, r):
        t, s = divmod(places[(kind, i, r)], SLOTS)
        return yroll(mixed[t][s % 2], -DEEP * s)

    return rim


def stream(get_h, get_f, hs_ref, sums_ref, a_ref, b_ref, rim_of_f):
    lane = lanes()
    wide = Wide(lane)
    sent = {"fore": [], "back": []}
    part = {"fore": [], "back": []}
    for i, v in enumerate(HV):
        pulled = [wide.pull(get_h(i, r), v) for r in range(2)]
        if v[0] == 0:
            put(hs_ref, i, 0, pulled[0])
            put(hs_ref, i, 1, pulled[1])
            part["fore"].append(pulled[1])
            part["back"].append(pulled[0])
        elif v[0] == 1:
            put(hs_ref, i, 1, pulled[0])
            sent["fore"].append(pulled[1])
            part["fore"].append(pulled[0])
        else:
            put(hs_ref, i, 0, pulled[1])
            sent["back"].append(pulled[0])
            part["back"].append(pulled[1])
    for n, way in enumerate(("fore", "back")):
        kept = functools.reduce(add, sent[way])
        sums_ref[n, 0] = kept[0]
        sums_ref[n, 1] = kept[1]
    for i in F_FORE:
        sent["fore"].append(wide.pull(get_f(i, 1), FV[i], rim_of_f))
    for i in F_BACK:
        sent["back"].append(wide.pull(get_f(i, 0), FV[i], rim_of_f))
    swap = odd("gx")
    packed = []
    for way in ("fore", "back"):
        fields = sent[way] + [functools.reduce(add, part[way])]
        rims = jnp.zeros((16, 128), F32)
        for j, field in enumerate(fields):
            if field[1] is not None:
                rims = jnp.where(lane // 8 == j, yroll(field[1], 8 * j + 4), rims)
        packed.append([field[0] for field in fields] + [rims])
    for j in range(SENT + 1):
        a_ref[j] = jnp.where(swap, packed[1][j], packed[0][j])
        b_ref[j] = jnp.where(swap, packed[0][j], packed[1][j])


def stream_rest(get_f, fs_ref):
    wide = Wide(lanes())
    for i, v in enumerate(FV):
        for r in range(2):
            if 0 <= r + v[0] < 2:
                put(fs_ref, i, r + v[0], wide.pull(get_f(i, r), v, fs_ref.shape[2] == 2))


def collide(hs_ref, fs_ref, sums_ref, a_ref, b_ref, solid_of, new_h, new_f, scratch, tiles, row_done=None):
    got_ref, phi_ref, grad_ref = scratch
    lane = lanes()
    wide = Wide(lane)
    swap = odd("gx")
    a, b = partner(a_ref, SENT, swap, True), partner(b_ref, SENT, swap, False)
    rims = jnp.where(swap, a, b), jnp.where(swap, b, a)
    for j in range(SENT):
        a, b = partner(a_ref, j, swap, True), partner(b_ref, j, swap, False)
        got_ref[0, j, 0] = jnp.where(swap, a, b)
        got_ref[1, j, 0] = jnp.where(swap, b, a)
        for n in range(2):
            got_ref[n, j, 1] = yroll(rims[n], -(8 * j + 4))

    def h_at(i, r, t, zs):
        if r == 0 and HV[i][0] == 1:
            return got_ref[0, H_FORE.index(i), t, zs]
        if r == 1 and HV[i][0] == -1:
            return got_ref[1, H_BACK.index(i), t, zs]
        return hs_ref[i, r, t, zs]

    def f_at(i, r, t, zs):
        if r == 0 and FV[i][0] == 1:
            return got_ref[0, len(H_FORE) + F_FORE.index(i), t, zs]
        if r == 1 and FV[i][0] == -1:
            return got_ref[1, len(H_BACK) + F_BACK.index(i), t, zs]
        return fs_ref[i, r, t, zs]

    every = slice(None)
    for t in range(2):
        phi_ref[0, t] = got_ref[0, SENT - 1, t] + sums_ref[1, t]
        phi_ref[3, t] = got_ref[1, SENT - 1, t] + sums_ref[0, t]
        for r in range(2):
            phi_ref[r + 1, t] = total(h_at(i, r, t, every) for i in range(NH))
    for r in range(2):
        below, own, above = [(phi_ref[q, 0], phi_ref[q, 1]) for q in (r, r + 1, r + 2)]
        across = (above[0] - below[0], above[1] - below[1])
        around = add(above, below)
        upright = tuple(zroll(own[t], 1) + zroll(own[t], -1) for t in range(2))
        third = tuple(
            (1.0 / 3.0) * own[t] + (1.0 / 6.0) * (around[t] + upright[t]) for t in range(2)
        )
        rim = tiles == 2
        third_up, third_down = wide.shift(third, -1, rim), wide.shift(third, 1, rim)
        across_up, across_down = wide.shift(across, -1, rim), wide.shift(across, 1, rim)
        own_up, own_down = wide.shift(own, -1, rim), wide.shift(own, 1, rim)
        for t in range(tiles):
            along_y = own_up[t] + own_down[t]
            level = (1.0 / 6.0) * own[t] + (1.0 / 12.0) * (around[t] + along_y)
            grad_ref[r, t, 0] = (1.0 / 6.0) * across[t] + (1.0 / 12.0) * (
                across_up[t] + across_down[t] + zroll(across[t], 1) + zroll(across[t], -1)
            )
            grad_ref[r, t, 1] = 0.5 * (third_up[t] - third_down[t])
            grad_ref[r, t, 2] = zroll(level, -1) - zroll(level, 1)
            grad_ref[r, t, 3] = (
                (1.0 / 3.0) * (around[t] + upright[t])
                + (1.0 / 6.0) * (zroll(around[t], 1) + zroll(around[t], -1))
                + (third_up[t] + third_down[t])
                - 4.0 * own[t]
            )
    for r in range(2):
        for t in range(tiles):
            for z in (0, 8):
                zs = slice(z, z + 8)
                solid = solid_of(r, t, zs)
                phi = phi_ref[r + 1, t, zs]
                grad = [grad_ref[r, t, n, zs] for n in range(3)]
                collide_part(
                    phi,
                    grad,
                    grad_ref[r, t, 3, zs],
                    solid,
                    lambda i, r=r, t=t, zs=zs: h_at(i, r, t, zs),
                    lambda i, r=r, t=t, zs=zs: f_at(i, r, t, zs),
                    functools.partial(new_h, r, t, zs),
                    functools.partial(new_f, r, t, zs),
                )
        if row_done is not None:
            row_done(r)


def dot(v, u):
    terms = [(s, c) for s, c in zip(v, u, strict=True) if s]
    out = None
    for s, c in terms:
        if out is None:
            out = c if s > 0 else -c
        else:
            out = out + c if s > 0 else out - c
    return out


def collide_part(phi, grad, laplacian, solid, h_at, f_at, put_h, put_f):
    clipped = jnp.clip(phi, 0.0, 1.0)
    density = 1.0 + 2.0 * clipped
    relax = 0.6 + 0.4 * clipped
    inverse = 1.0 / (density * relax)
    rate, per_density = density * inverse, relax * inverse
    potential = (4.0 * BETA) * phi * (phi - 1.0) * (phi - 0.5) - KAPPA * laplacian
    force = [potential * g for g in grad]
    squared = grad[0] * grad[0] + grad[1] * grad[1] + grad[2] * grad[2]
    scale = 1.0 / jnp.maximum(jnp.sqrt(squared), FLOOR)
    f_rest = f_at(0)
    moment = [0.5 * c for c in force]
    pressure = f_rest
    for i, o in FP:
        fi, fo = f_at(i), f_at(o)
        difference = fi - fo
        pressure = pressure + (fi + fo)
        for n in range(3):
            if FV[i][n]:
                moment[n] = (
                    moment[n] + difference if FV[i][n] > 0 else moment[n] - difference
                )
    u = [m * per_density for m in moment]
    speed = u[0] * u[0] + u[1] * u[1] + u[2] * u[2]
    pull = 3.0 * (1.0 - 0.5 * rate) * per_density
    drive = [3.0 * rate * u[n] + pull * force[n] for n in range(3)]
    keep = 1.0 - rate
    level = rate * (pressure - 1.5 * speed)
    bend = 4.5 * rate
    put_f(0, jnp.where(solid, f_rest, keep * f_rest + FW[0] * level))
    for i, o in FP:
        w = FW[i]
        fi, fo = f_at(i), f_at(o)
        along = dot(FV[i], u)
        even = w * (level + bend * (along * along))
        uneven = w * dot(FV[i], drive)
        put_f(i, jnp.where(solid, fo, keep * fi + (even + uneven)))
        put_f(o, jnp.where(solid, fi, keep * fo + (even - uneven)))
    sharp = LAMBDA * phi * (1.0 - phi) * scale
    drift = [3.0 * phi * u[n] + sharp * grad[n] for n in range(3)]
    h_rest = h_at(0)
    stay = 1.0 - INV_RELAX
    put_h(0, jnp.where(solid, h_rest, stay * h_rest + (INV_RELAX * HW[0]) * phi))
    for i, o in HP:
        w = INV_RELAX * HW[i]
        hi, ho = h_at(i), h_at(o)
        even = w * phi
        uneven = w * dot(HV[i], drift)
        put_h(i, jnp.where(solid, ho, stay * hi + (even + uneven)))
        put_h(o, jnp.where(solid, hi, stay * ho + (even - uneven)))


def first_kernel(h_ref, f_ref, s_ref, ya_ref, yb_ref, a_ref, b_ref, hs_ref, sums_ref, so_ref):
    rim = spread_edges(ya_ref, yb_ref)
    for r in range(2):
        so_ref[r, 0] = (s_ref[r] > 0).astype(F32)
        so_ref[r, 1] = rim("s", 0, r)
    stream(
        lambda i, r: (h_ref[i, r], rim("h", i, r)),
        lambda i, r: (f_ref[i, r], rim("f", i, r)),
        hs_ref,
        sums_ref,
        a_ref,
        b_ref,
        True,
    )


def middle_kernel(
    hs_ref, f_ref, ya_ref, yb_ref, sums_ref, s_ref, ra_ref, rb_ref,
    a_ref, b_ref, hs2_ref, sums2_ref, f1_ref,
    h1_ref, fs_ref, got_ref, phi_ref, grad_ref,
):
    rim = spread_edges(ya_ref, yb_ref)
    stream_rest(lambda i, r: (f_ref[i, r], rim("f", i, r)), fs_ref)

    def new_h(r, t, zs, i, value):
        h1_ref[i, r, t, zs] = value

    def new_f(r, t, zs, i, value):
        f1_ref[i, r, t, zs] = value

    collide(
        hs_ref,
        fs_ref,
        sums_ref,
        ra_ref,
        rb_ref,
        lambda r, t, zs: s_ref[r, t, zs] > 0.5,
        new_h,
        new_f,
        (got_ref, phi_ref, grad_ref),
        2,
    )
    stream(
        lambda i, r: (h1_ref[i, r, 0], h1_ref[i, r, 1]),
        lambda i, r: (f1_ref[i, r, 0], f1_ref[i, r, 1]),
        hs2_ref,
        sums2_ref,
        a_ref,
        b_ref,
        False,
    )


def last_kernel(
    hs_ref, f1_ref, sums_ref, s_ref, ra_ref, rb_ref,
    h_hbm, f_hbm,
    h_ref, f_ref, fs_ref, got_ref, phi_ref, grad_ref, sems,
):
    stream_rest(lambda i, r: (f1_ref[i, r, 0], f1_ref[i, r, 1]), fs_ref)

    def new_h(r, t, zs, i, value):
        h_ref[r, i, zs] = value

    def new_f(r, t, zs, i, value):
        f_ref[r, i, zs] = value

    copies = []

    def row_done(r):
        for n, (source, target) in enumerate(((h_ref, h_hbm), (f_ref, f_hbm))):
            copies.append(
                pltpu.make_async_copy(source.at[r], target.at[:, r], sems.at[r, n])
            )
            copies[-1].start()

    collide(
        hs_ref,
        fs_ref,
        sums_ref,
        ra_ref,
        rb_ref,
        lambda r, t, zs: s_ref[r, t, zs] > 0.5,
        new_h,
        new_f,
        (got_ref, phi_ref, grad_ref),
        1,
        row_done,
    )
    for copy in copies:
        copy.wait()


HBM = pl.BlockSpec(memory_space=pltpu.HBM)
VMEM = pl.BlockSpec(memory_space=pltpu.VMEM)
TILE = (16, 128)
COVER = pl.CostEstimate(flops=2_000_000_000, bytes_accessed=4_000_000, transcendentals=0)
LIMIT = 16 * 1024 * 1024
NEAR_Y, FAR_Y, NEAR_X, FAR_X = True, True, True, False


def call(kernel, outs, *args, scratch=(), sems=None, source=VMEM, target=VMEM, cost=None):
    kept = [pltpu.VMEM(shape, F32) for shape in scratch]
    if sems is not None:
        kept.append(pltpu.SemaphoreType.DMA(sems))
    return pl.pallas_call(
        kernel,
        out_shape=[
            out if hasattr(out, "dtype") else jax.ShapeDtypeStruct(out, F32)
            for out in outs
        ],
        in_specs=[source] * len(args),
        out_specs=[target] * len(outs),
        scratch_shapes=kept,
        compiler_params=pltpu.CompilerParams(vmem_limit_bytes=LIMIT),
        cost_estimate=cost,
    )(*args)


def swap_near(block, axis, gather):
    n = lax.axis_size(axis)
    if gather:
        groups = [[i, i + 1] for i in range(0, n, 2)]
        return lax.all_gather(block, axis, axis_index_groups=groups)
    return lax.ppermute(block, axis, [(i, i ^ 1) for i in range(n)])


def swap_far(block, axis, gather):
    n = lax.axis_size(axis)
    if gather:
        groups = [[i, (i + 1) % n] for i in range(1, n, 2)]
        return lax.all_gather(block, axis, axis_index_groups=groups)
    route = [(i, (i + 1) % n if i % 2 else (i - 1) % n) for i in range(n)]
    return lax.ppermute(block, axis, route)


def shards(phase_pops, flow_pops, solid_flags):
    edge, sent = (EDGE_TILES, *TILE), (SENT + 1, *TILE)
    wide_h, wide_f = (NH, 2, 2, *TILE), (NF, 2, 2, *TILE)
    sums = (2, 2, *TILE)
    scratch = [(2, SENT, 2, *TILE), (4, 2, *TILE), (2, 2, 4, *TILE)]
    h, f = phase_pops, flow_pops
    (slot,) = call(slots_kernel, [jax.ShapeDtypeStruct(TILE, jnp.int32)], cost=COVER)
    a, b = call(edges_kernel, [edge, edge], slot, h, f, solid_flags)
    ya, yb = swap_near(a, "gy", NEAR_Y), swap_far(b, "gy", FAR_Y)
    a, b, hs, kept, solid = call(
        first_kernel, [sent, sent, wide_h, sums, (2, 2, *TILE)], h, f, solid_flags, ya, yb
    )
    a, b = swap_near(a, "gx", NEAR_X), swap_far(b, "gx", FAR_X)
    a, b, hs, kept, f = call(
        middle_kernel,
        [sent, sent, wide_h, sums, wide_f],
        *(hs, f, ya, yb, kept, solid, a, b),
        scratch=[wide_h, wide_f, *scratch],
    )
    a, b = swap_near(a, "gx", NEAR_X), swap_far(b, "gx", FAR_X)
    out_h, out_f = (NH, 2, *TILE), (NF, 2, *TILE)
    return tuple(
        call(
            last_kernel,
            [out_h, out_f],
            *(hs, f, kept, solid, a, b),
            scratch=[(2, NH, *TILE), (2, NF, *TILE), (NF, 2, 1, *TILE), *scratch],
            sems=(2, 2),
            target=HBM,
        )
    )


def solution(mesh):
    placed = (P(None, "gx", None, "gy"), P(None, "gx", None, "gy"), P("gx", None, "gy"))
    return jax.shard_map(
        shards,
        mesh=mesh,
        in_specs=placed,
        out_specs=placed[:2],
        check_vma=False,
    )
```

```python
import functools

import jax
import jax.numpy as jnp
from jax import lax
from jax.experimental import pallas as pl
from jax.experimental.pallas import tpu as pltpu
from jax.sharding import PartitionSpec as P

HV = [
    (0, 0, 0),
    (1, 0, 0),
    (-1, 0, 0),
    (0, 1, 0),
    (0, -1, 0),
    (0, 0, 1),
    (0, 0, -1),
    (1, 1, 1),
    (1, 1, -1),
    (1, -1, 1),
    (1, -1, -1),
    (-1, 1, 1),
    (-1, 1, -1),
    (-1, -1, 1),
    (-1, -1, -1),
]
HW = [2.0 / 9.0] + [1.0 / 9.0] * 6 + [1.0 / 72.0] * 8
FV = [
    (0, 0, 0),
    (1, 0, 0),
    (-1, 0, 0),
    (0, 1, 0),
    (0, -1, 0),
    (0, 0, 1),
    (0, 0, -1),
    (1, 1, 0),
    (1, -1, 0),
    (-1, 1, 0),
    (-1, -1, 0),
    (1, 0, 1),
    (1, 0, -1),
    (-1, 0, 1),
    (-1, 0, -1),
    (0, 1, 1),
    (0, 1, -1),
    (0, -1, 1),
    (0, -1, -1),
]
FW = [1.0 / 3.0] + [1.0 / 18.0] * 6 + [1.0 / 36.0] * 12
NH, NF = len(HV), len(FV)
BETA = 12.0 * 0.05 / 4.0
KAPPA = 1.5 * 0.05 * 4.0
FLOOR = 0.1
LAMBDA = 0.3
INV_RELAX = 1.0 / 0.8


def neg(v):
    return (-v[0], -v[1], -v[2])


def pairs(velocities):
    return [
        (i, velocities.index(neg(v))) for i, v in enumerate(velocities) if v > neg(v)
    ]


HP, FP = pairs(HV), pairs(FV)
H_FORE = [i for i, v in enumerate(HV) if v[0] == 1]
H_BACK = [i for i, v in enumerate(HV) if v[0] == -1]
F_FORE = [i for i, v in enumerate(FV) if v[0] == 1]
F_BACK = [i for i, v in enumerate(FV) if v[0] == -1]
DEEP = 4
SLOTS = 128 // DEEP
ROWS = [("h", i, r) for i in range(NH) for r in range(2)] + [
    ("f", i, r) for i in range(NF) for r in range(2)
] + [("s", 0, r) for r in range(2)]
EDGE_TILES = -(-len(ROWS) // SLOTS)
SENT = len(H_FORE) + len(F_FORE) + 1
F32 = jnp.float32


def lanes():
    return lax.broadcasted_iota(jnp.int32, (16, 128), 1)


def yroll(tile, shift):
    return pltpu.roll(tile, shift % 128, axis=1)


def zroll(tile, shift):
    return pltpu.roll(tile, shift % 16, axis=0)


def odd(axis):
    return lax.rem(lax.axis_index(axis), 2) == 1


def partner(ref, j, swap, near):
    if len(ref.shape) == 3:
        return ref[j]
    first, second = ref[0, j], ref[1, j]
    return jnp.where(swap, first, second) if near else jnp.where(swap, second, first)


def total(terms):
    terms = list(terms)
    while len(terms) > 1:
        terms = [
            terms[k] + terms[k + 1] if k + 1 < len(terms) else terms[k]
            for k in range(0, len(terms), 2)
        ]
    return terms[0]


def put(ref, i, r, field):
    for t in range(ref.shape[2]):
        ref[i, r, t] = field[t]


class Wide:
    def __init__(self, lane):
        self.first, self.last = lane == 0, lane == 127

    def shift(self, field, c, rim=True):
        if c == 0:
            return field
        edge = self.first if c == 1 else self.last
        own, out = yroll(field[0], c), yroll(field[1], c)
        return (
            jnp.where(edge, out, own),
            jnp.where(edge, own, out) if rim else None,
        )

    def pull(self, field, v, rim=True):
        if v[2]:
            field = (zroll(field[0], v[2]), zroll(field[1], v[2]))
        return self.shift(field, v[1], rim)


def add(a, b):
    return (a[0] + b[0], a[1] + b[1])


def slots_kernel(slot_ref):
    slot_ref[...] = lanes() // DEEP


def edges_kernel(slot_ref, h_ref, f_ref, s_ref, a_ref, b_ref):
    slot = slot_ref[...]
    right = [jnp.zeros((16, 128), F32) for _ in range(EDGE_TILES)]
    left = [jnp.zeros((16, 128), F32) for _ in range(EDGE_TILES)]
    for k, (kind, i, r) in enumerate(ROWS):
        t, s = divmod(k, SLOTS)
        if kind == "s":
            source = (s_ref[r] > 0).astype(F32)
        else:
            source = h_ref[i, r] if kind == "h" else f_ref[i, r]
        turned = yroll(source, DEEP * (s + 1))
        right[t] = jnp.where(slot == s, turned, right[t])
        left[t] = jnp.where(slot == (s + 1) % SLOTS, turned, left[t])
    swap = odd("gy")
    for t in range(EDGE_TILES):
        left_tile = yroll(left[t], -DEEP)
        a_ref[t] = jnp.where(swap, left_tile, right[t])
        b_ref[t] = jnp.where(swap, right[t], left_tile)


def spread_edges(a_ref, b_ref):
    lane = lanes()
    even_slot = lax.rem(lane // DEEP, 2) == 0
    swap = odd("gy")
    mixed = []
    for t in range(EDGE_TILES):
        a, b = partner(a_ref, t, swap, True), partner(b_ref, t, swap, False)
        after = jnp.where(swap, b, a)
        before = yroll(jnp.where(swap, a, b), -DEEP)
        mixed.append(
            (jnp.where(even_slot, after, before), jnp.where(even_slot, before, after))
        )
    places = {row: k for k, row in enumerate(ROWS)}

    def rim(kind, i, r):
        t, s = divmod(places[(kind, i, r)], SLOTS)
        return yroll(mixed[t][s % 2], -DEEP * s)

    return rim


def stream(get_h, get_f, hs_ref, sums_ref, a_ref, b_ref, rim_of_f):
    lane = lanes()
    wide = Wide(lane)
    sent = {"fore": [], "back": []}
    part = {"fore": [], "back": []}
    for i, v in enumerate(HV):
        pulled = [wide.pull(get_h(i, r), v) for r in range(2)]
        if v[0] == 0:
            put(hs_ref, i, 0, pulled[0])
            put(hs_ref, i, 1, pulled[1])
            part["fore"].append(pulled[1])
            part["back"].append(pulled[0])
        elif v[0] == 1:
            put(hs_ref, i, 1, pulled[0])
            sent["fore"].append(pulled[1])
            part["fore"].append(pulled[0])
        else:
            put(hs_ref, i, 0, pulled[1])
            sent["back"].append(pulled[0])
            part["back"].append(pulled[1])
    for n, way in enumerate(("fore", "back")):
        kept = functools.reduce(add, sent[way])
        sums_ref[n, 0] = kept[0]
        sums_ref[n, 1] = kept[1]
    for i in F_FORE:
        sent["fore"].append(wide.pull(get_f(i, 1), FV[i], rim_of_f))
    for i in F_BACK:
        sent["back"].append(wide.pull(get_f(i, 0), FV[i], rim_of_f))
    swap = odd("gx")
    packed = []
    for way in ("fore", "back"):
        fields = sent[way] + [functools.reduce(add, part[way])]
        rims = jnp.zeros((16, 128), F32)
        for j, field in enumerate(fields):
            if field[1] is not None:
                rims = jnp.where(lane // 8 == j, yroll(field[1], 8 * j + 4), rims)
        packed.append([field[0] for field in fields] + [rims])
    for j in range(SENT + 1):
        a_ref[j] = jnp.where(swap, packed[1][j], packed[0][j])
        b_ref[j] = jnp.where(swap, packed[0][j], packed[1][j])


def stream_rest(get_f, fs_ref):
    wide = Wide(lanes())
    for i, v in enumerate(FV):
        for r in range(2):
            if 0 <= r + v[0] < 2:
                put(fs_ref, i, r + v[0], wide.pull(get_f(i, r), v, fs_ref.shape[2] == 2))


def collide(hs_ref, fs_ref, sums_ref, a_ref, b_ref, solid_of, new_h, new_f, scratch, tiles, row_done=None):
    got_ref, phi_ref, grad_ref = scratch
    lane = lanes()
    wide = Wide(lane)
    swap = odd("gx")
    a, b = partner(a_ref, SENT, swap, True), partner(b_ref, SENT, swap, False)
    rims = jnp.where(swap, a, b), jnp.where(swap, b, a)
    for j in range(SENT):
        a, b = partner(a_ref, j, swap, True), partner(b_ref, j, swap, False)
        got_ref[0, j, 0] = jnp.where(swap, a, b)
        got_ref[1, j, 0] = jnp.where(swap, b, a)
        for n in range(2):
            got_ref[n, j, 1] = yroll(rims[n], -(8 * j + 4))

    def h_at(i, r, t, zs):
        if r == 0 and HV[i][0] == 1:
            return got_ref[0, H_FORE.index(i), t, zs]
        if r == 1 and HV[i][0] == -1:
            return got_ref[1, H_BACK.index(i), t, zs]
        return hs_ref[i, r, t, zs]

    def f_at(i, r, t, zs):
        if r == 0 and FV[i][0] == 1:
            return got_ref[0, len(H_FORE) + F_FORE.index(i), t, zs]
        if r == 1 and FV[i][0] == -1:
            return got_ref[1, len(H_BACK) + F_BACK.index(i), t, zs]
        return fs_ref[i, r, t, zs]

    every = slice(None)
    for t in range(2):
        phi_ref[0, t] = got_ref[0, SENT - 1, t] + sums_ref[1, t]
        phi_ref[3, t] = got_ref[1, SENT - 1, t] + sums_ref[0, t]
        for r in range(2):
            phi_ref[r + 1, t] = total(h_at(i, r, t, every) for i in range(NH))
    for r in range(2):
        below, own, above = [(phi_ref[q, 0], phi_ref[q, 1]) for q in (r, r + 1, r + 2)]
        across = (above[0] - below[0], above[1] - below[1])
        around = add(above, below)
        upright = tuple(zroll(own[t], 1) + zroll(own[t], -1) for t in range(2))
        third = tuple(
            (1.0 / 3.0) * own[t] + (1.0 / 6.0) * (around[t] + upright[t]) for t in range(2)
        )
        rim = tiles == 2
        third_up, third_down = wide.shift(third, -1, rim), wide.shift(third, 1, rim)
        across_up, across_down = wide.shift(across, -1, rim), wide.shift(across, 1, rim)
        own_up, own_down = wide.shift(own, -1, rim), wide.shift(own, 1, rim)
        for t in range(tiles):
            along_y = own_up[t] + own_down[t]
            level = (1.0 / 6.0) * own[t] + (1.0 / 12.0) * (around[t] + along_y)
            grad_ref[r, t, 0] = (1.0 / 6.0) * across[t] + (1.0 / 12.0) * (
                across_up[t] + across_down[t] + zroll(across[t], 1) + zroll(across[t], -1)
            )
            grad_ref[r, t, 1] = 0.5 * (third_up[t] - third_down[t])
            grad_ref[r, t, 2] = zroll(level, -1) - zroll(level, 1)
            grad_ref[r, t, 3] = (
                (1.0 / 3.0) * (around[t] + upright[t])
                + (1.0 / 6.0) * (zroll(around[t], 1) + zroll(around[t], -1))
                + (third_up[t] + third_down[t])
                - 4.0 * own[t]
            )
    for r in range(2):
        for t in range(tiles):
            for z in (0, 8):
                zs = slice(z, z + 8)
                solid = solid_of(r, t, zs)
                phi = phi_ref[r + 1, t, zs]
                grad = [grad_ref[r, t, n, zs] for n in range(3)]
                collide_part(
                    phi,
                    grad,
                    grad_ref[r, t, 3, zs],
                    solid,
                    lambda i, r=r, t=t, zs=zs: h_at(i, r, t, zs),
                    lambda i, r=r, t=t, zs=zs: f_at(i, r, t, zs),
                    functools.partial(new_h, r, t, zs),
                    functools.partial(new_f, r, t, zs),
                )
        if row_done is not None:
            row_done(r)


def dot(v, u):
    terms = [(s, c) for s, c in zip(v, u, strict=True) if s]
    out = None
    for s, c in terms:
        if out is None:
            out = c if s > 0 else -c
        else:
            out = out + c if s > 0 else out - c
    return out


def collide_part(phi, grad, laplacian, solid, h_at, f_at, put_h, put_f):
    clipped = jnp.clip(phi, 0.0, 1.0)
    density = 1.0 + 2.0 * clipped
    relax = 0.6 + 0.4 * clipped
    inverse = 1.0 / (density * relax)
    rate, per_density = density * inverse, relax * inverse
    potential = (4.0 * BETA) * phi * (phi - 1.0) * (phi - 0.5) - KAPPA * laplacian
    force = [potential * g for g in grad]
    squared = grad[0] * grad[0] + grad[1] * grad[1] + grad[2] * grad[2]
    scale = 1.0 / jnp.maximum(jnp.sqrt(squared), FLOOR)
    f_rest = f_at(0)
    moment = [0.5 * c for c in force]
    pressure = f_rest
    for i, o in FP:
        fi, fo = f_at(i), f_at(o)
        difference = fi - fo
        pressure = pressure + (fi + fo)
        for n in range(3):
            if FV[i][n]:
                moment[n] = (
                    moment[n] + difference if FV[i][n] > 0 else moment[n] - difference
                )
    u = [m * per_density for m in moment]
    speed = u[0] * u[0] + u[1] * u[1] + u[2] * u[2]
    pull = 3.0 * (1.0 - 0.5 * rate) * per_density
    drive = [3.0 * rate * u[n] + pull * force[n] for n in range(3)]
    keep = 1.0 - rate
    level = rate * (pressure - 1.5 * speed)
    bend = 4.5 * rate
    put_f(0, jnp.where(solid, f_rest, keep * f_rest + FW[0] * level))
    for i, o in FP:
        w = FW[i]
        fi, fo = f_at(i), f_at(o)
        along = dot(FV[i], u)
        even = w * (level + bend * (along * along))
        uneven = w * dot(FV[i], drive)
        put_f(i, jnp.where(solid, fo, keep * fi + (even + uneven)))
        put_f(o, jnp.where(solid, fi, keep * fo + (even - uneven)))
    sharp = LAMBDA * phi * (1.0 - phi) * scale
    drift = [3.0 * phi * u[n] + sharp * grad[n] for n in range(3)]
    h_rest = h_at(0)
    stay = 1.0 - INV_RELAX
    put_h(0, jnp.where(solid, h_rest, stay * h_rest + (INV_RELAX * HW[0]) * phi))
    for i, o in HP:
        w = INV_RELAX * HW[i]
        hi, ho = h_at(i), h_at(o)
        even = w * phi
        uneven = w * dot(HV[i], drift)
        put_h(i, jnp.where(solid, ho, stay * hi + (even + uneven)))
        put_h(o, jnp.where(solid, hi, stay * ho + (even - uneven)))


def first_kernel(h_ref, f_ref, s_ref, ya_ref, yb_ref, a_ref, b_ref, hs_ref, sums_ref, so_ref):
    rim = spread_edges(ya_ref, yb_ref)
    for r in range(2):
        so_ref[r, 0] = (s_ref[r] > 0).astype(F32)
        so_ref[r, 1] = rim("s", 0, r)
    stream(
        lambda i, r: (h_ref[i, r], rim("h", i, r)),
        lambda i, r: (f_ref[i, r], rim("f", i, r)),
        hs_ref,
        sums_ref,
        a_ref,
        b_ref,
        True,
    )


def first_rest_kernel(f_ref, ya_ref, yb_ref, fs_ref):
    rim = spread_edges(ya_ref, yb_ref)
    stream_rest(lambda i, r: (f_ref[i, r], rim("f", i, r)), fs_ref)


def middle_kernel(
    hs_ref, fs_ref, sums_ref, s_ref, ra_ref, rb_ref,
    a_ref, b_ref, hs2_ref, sums2_ref, f1_ref,
    h1_ref, got_ref, phi_ref, grad_ref,
):
    def new_h(r, t, zs, i, value):
        h1_ref[i, r, t, zs] = value

    def new_f(r, t, zs, i, value):
        f1_ref[i, r, t, zs] = value

    collide(
        hs_ref,
        fs_ref,
        sums_ref,
        ra_ref,
        rb_ref,
        lambda r, t, zs: s_ref[r, t, zs] > 0.5,
        new_h,
        new_f,
        (got_ref, phi_ref, grad_ref),
        2,
    )
    stream(
        lambda i, r: (h1_ref[i, r, 0], h1_ref[i, r, 1]),
        lambda i, r: (f1_ref[i, r, 0], f1_ref[i, r, 1]),
        hs2_ref,
        sums2_ref,
        a_ref,
        b_ref,
        False,
    )


def last_kernel(
    hs_ref, f1_ref, sums_ref, s_ref, ra_ref, rb_ref,
    h_hbm, f_hbm,
    h_ref, f_ref, fs_ref, got_ref, phi_ref, grad_ref, sems,
):
    stream_rest(lambda i, r: (f1_ref[i, r, 0], f1_ref[i, r, 1]), fs_ref)

    def new_h(r, t, zs, i, value):
        h_ref[r, i, zs] = value

    def new_f(r, t, zs, i, value):
        f_ref[r, i, zs] = value

    copies = []

    def row_done(r):
        for n, (source, target) in enumerate(((h_ref, h_hbm), (f_ref, f_hbm))):
            copies.append(
                pltpu.make_async_copy(source.at[r], target.at[:, r], sems.at[r, n])
            )
            copies[-1].start()

    collide(
        hs_ref,
        fs_ref,
        sums_ref,
        ra_ref,
        rb_ref,
        lambda r, t, zs: s_ref[r, t, zs] > 0.5,
        new_h,
        new_f,
        (got_ref, phi_ref, grad_ref),
        1,
        row_done,
    )
    for copy in copies:
        copy.wait()


HBM = pl.BlockSpec(memory_space=pltpu.HBM)
VMEM = pl.BlockSpec(memory_space=pltpu.VMEM)
TILE = (16, 128)
COVER = pl.CostEstimate(flops=2_000_000_000, bytes_accessed=4_000_000, transcendentals=0)
LIMIT = 16 * 1024 * 1024
NEAR_Y, FAR_Y, NEAR_X, FAR_X = True, True, True, False


def call(kernel, outs, *args, scratch=(), sems=None, source=VMEM, target=VMEM, cost=None):
    kept = [pltpu.VMEM(shape, F32) for shape in scratch]
    if sems is not None:
        kept.append(pltpu.SemaphoreType.DMA(sems))
    return pl.pallas_call(
        kernel,
        out_shape=[
            out if hasattr(out, "dtype") else jax.ShapeDtypeStruct(out, F32)
            for out in outs
        ],
        in_specs=[source] * len(args),
        out_specs=[target] * len(outs),
        scratch_shapes=kept,
        compiler_params=pltpu.CompilerParams(vmem_limit_bytes=LIMIT),
        cost_estimate=cost,
    )(*args)


def swap_near(block, axis, gather):
    n = lax.axis_size(axis)
    if gather:
        groups = [[i, i + 1] for i in range(0, n, 2)]
        return lax.all_gather(block, axis, axis_index_groups=groups)
    return lax.ppermute(block, axis, [(i, i ^ 1) for i in range(n)])


def swap_far(block, axis, gather):
    n = lax.axis_size(axis)
    if gather:
        groups = [[i, (i + 1) % n] for i in range(1, n, 2)]
        return lax.all_gather(block, axis, axis_index_groups=groups)
    route = [(i, (i + 1) % n if i % 2 else (i - 1) % n) for i in range(n)]
    return lax.ppermute(block, axis, route)


def shards(phase_pops, flow_pops, solid_flags):
    edge, sent = (EDGE_TILES, *TILE), (SENT + 1, *TILE)
    wide_h, wide_f = (NH, 2, 2, *TILE), (NF, 2, 2, *TILE)
    sums = (2, 2, *TILE)
    scratch = [(2, SENT, 2, *TILE), (4, 2, *TILE), (2, 2, 4, *TILE)]
    h, f = phase_pops, flow_pops
    (slot,) = call(slots_kernel, [jax.ShapeDtypeStruct(TILE, jnp.int32)], cost=COVER)
    a, b = call(edges_kernel, [edge, edge], slot, h, f, solid_flags)
    ya, yb = swap_near(a, "gy", NEAR_Y), swap_far(b, "gy", FAR_Y)
    a, b, hs, kept, solid = call(
        first_kernel, [sent, sent, wide_h, sums, (2, 2, *TILE)], h, f, solid_flags, ya, yb
    )
    a, b = swap_near(a, "gx", NEAR_X), swap_far(b, "gx", FAR_X)
    (fs,) = call(first_rest_kernel, [wide_f], f, ya, yb)
    a, b, hs, kept, f = call(
        middle_kernel,
        [sent, sent, wide_h, sums, wide_f],
        *(hs, fs, kept, solid, a, b),
        scratch=[wide_h, *scratch],
    )
    a, b = swap_near(a, "gx", NEAR_X), swap_far(b, "gx", FAR_X)
    out_h, out_f = (NH, 2, *TILE), (NF, 2, *TILE)
    return tuple(
        call(
            last_kernel,
            [out_h, out_f],
            *(hs, f, kept, solid, a, b),
            scratch=[(2, NH, *TILE), (2, NF, *TILE), (NF, 2, 1, *TILE), *scratch],
            sems=(2, 2),
            target=HBM,
        )
    )


def solution(mesh):
    placed = (P(None, "gx", None, "gy"), P(None, "gx", None, "gy"), P("gx", None, "gy"))
    return jax.shard_map(
        shards,
        mesh=mesh,
        in_specs=placed,
        out_specs=placed[:2],
        check_vma=False,
    )
```

```python
import functools

import jax
import jax.numpy as jnp
from jax import lax
from jax.experimental import pallas as pl
from jax.experimental.pallas import tpu as pltpu
from jax.sharding import PartitionSpec as P

HV = [
    (0, 0, 0),
    (1, 0, 0),
    (-1, 0, 0),
    (0, 1, 0),
    (0, -1, 0),
    (0, 0, 1),
    (0, 0, -1),
    (1, 1, 1),
    (1, 1, -1),
    (1, -1, 1),
    (1, -1, -1),
    (-1, 1, 1),
    (-1, 1, -1),
    (-1, -1, 1),
    (-1, -1, -1),
]
HW = [2.0 / 9.0] + [1.0 / 9.0] * 6 + [1.0 / 72.0] * 8
FV = [
    (0, 0, 0),
    (1, 0, 0),
    (-1, 0, 0),
    (0, 1, 0),
    (0, -1, 0),
    (0, 0, 1),
    (0, 0, -1),
    (1, 1, 0),
    (1, -1, 0),
    (-1, 1, 0),
    (-1, -1, 0),
    (1, 0, 1),
    (1, 0, -1),
    (-1, 0, 1),
    (-1, 0, -1),
    (0, 1, 1),
    (0, 1, -1),
    (0, -1, 1),
    (0, -1, -1),
]
FW = [1.0 / 3.0] + [1.0 / 18.0] * 6 + [1.0 / 36.0] * 12
NH, NF = len(HV), len(FV)
BETA = 12.0 * 0.05 / 4.0
KAPPA = 1.5 * 0.05 * 4.0
FLOOR = 0.1
LAMBDA = 0.3
INV_RELAX = 1.0 / 0.8


def neg(v):
    return (-v[0], -v[1], -v[2])


def pairs(velocities):
    return [
        (i, velocities.index(neg(v))) for i, v in enumerate(velocities) if v > neg(v)
    ]


HP, FP = pairs(HV), pairs(FV)
H_FORE = [i for i, v in enumerate(HV) if v[0] == 1]
H_BACK = [i for i, v in enumerate(HV) if v[0] == -1]
F_FORE = [i for i, v in enumerate(FV) if v[0] == 1]
F_BACK = [i for i, v in enumerate(FV) if v[0] == -1]
DEEP = 4
SLOTS = 128 // DEEP
ROWS = [("h", i, r) for i in range(NH) for r in range(2)] + [
    ("f", i, r) for i in range(NF) for r in range(2)
] + [("s", 0, r) for r in range(2)]
EDGE_TILES = -(-len(ROWS) // SLOTS)
SENT = len(H_FORE) + len(F_FORE) + 1
F32 = jnp.float32


def lanes():
    return lax.broadcasted_iota(jnp.int32, (16, 128), 1)


def yroll(tile, shift):
    return pltpu.roll(tile, shift % 128, axis=1)


def zroll(tile, shift):
    return pltpu.roll(tile, shift % 16, axis=0)


def odd(axis):
    return lax.rem(lax.axis_index(axis), 2) == 1


def partner(ref, j, swap, near):
    if len(ref.shape) == 3:
        return ref[j]
    first, second = ref[0, j], ref[1, j]
    return jnp.where(swap, first, second) if near else jnp.where(swap, second, first)


def total(terms):
    terms = list(terms)
    while len(terms) > 1:
        terms = [
            terms[k] + terms[k + 1] if k + 1 < len(terms) else terms[k]
            for k in range(0, len(terms), 2)
        ]
    return terms[0]


def put(ref, i, r, field):
    for t in range(ref.shape[2]):
        ref[i, r, t] = field[t]


class Wide:
    def __init__(self, lane):
        self.first, self.last = lane == 0, lane == 127

    def shift(self, field, c, rim=True):
        if c == 0:
            return field
        edge = self.first if c == 1 else self.last
        own, out = yroll(field[0], c), yroll(field[1], c)
        return (
            jnp.where(edge, out, own),
            jnp.where(edge, own, out) if rim else None,
        )

    def pull(self, field, v, rim=True):
        if v[2]:
            field = (zroll(field[0], v[2]), zroll(field[1], v[2]))
        return self.shift(field, v[1], rim)


def add(a, b):
    return (a[0] + b[0], a[1] + b[1])


def slots_kernel(slot_ref):
    slot_ref[...] = lanes() // DEEP


def edges_kernel(slot_ref, h_ref, f_ref, s_ref, a_ref, b_ref):
    slot = slot_ref[...]
    right = [jnp.zeros((16, 128), F32) for _ in range(EDGE_TILES)]
    left = [jnp.zeros((16, 128), F32) for _ in range(EDGE_TILES)]
    for k, (kind, i, r) in enumerate(ROWS):
        t, s = divmod(k, SLOTS)
        if kind == "s":
            source = (s_ref[r] > 0).astype(F32)
        else:
            source = h_ref[i, r] if kind == "h" else f_ref[i, r]
        turned = yroll(source, DEEP * (s + 1))
        right[t] = jnp.where(slot == s, turned, right[t])
        left[t] = jnp.where(slot == (s + 1) % SLOTS, turned, left[t])
    swap = odd("gy")
    for t in range(EDGE_TILES):
        left_tile = yroll(left[t], -DEEP)
        a_ref[t] = jnp.where(swap, left_tile, right[t])
        b_ref[t] = jnp.where(swap, right[t], left_tile)


def spread_edges(a_ref, b_ref):
    lane = lanes()
    even_slot = lax.rem(lane // DEEP, 2) == 0
    swap = odd("gy")
    mixed = []
    for t in range(EDGE_TILES):
        a, b = partner(a_ref, t, swap, True), partner(b_ref, t, swap, False)
        after = jnp.where(swap, b, a)
        before = yroll(jnp.where(swap, a, b), -DEEP)
        mixed.append(
            (jnp.where(even_slot, after, before), jnp.where(even_slot, before, after))
        )
    places = {row: k for k, row in enumerate(ROWS)}

    def rim(kind, i, r):
        t, s = divmod(places[(kind, i, r)], SLOTS)
        return yroll(mixed[t][s % 2], -DEEP * s)

    return rim


def stream(get_h, get_f, hs_ref, sums_ref, a_ref, b_ref, rim_of_f):
    lane = lanes()
    wide = Wide(lane)
    sent = {"fore": [], "back": []}
    part = {"fore": [], "back": []}
    for i, v in enumerate(HV):
        pulled = [wide.pull(get_h(i, r), v) for r in range(2)]
        if v[0] == 0:
            put(hs_ref, i, 0, pulled[0])
            put(hs_ref, i, 1, pulled[1])
            part["fore"].append(pulled[1])
            part["back"].append(pulled[0])
        elif v[0] == 1:
            put(hs_ref, i, 1, pulled[0])
            sent["fore"].append(pulled[1])
            part["fore"].append(pulled[0])
        else:
            put(hs_ref, i, 0, pulled[1])
            sent["back"].append(pulled[0])
            part["back"].append(pulled[1])
    for n, way in enumerate(("fore", "back")):
        kept = functools.reduce(add, sent[way])
        sums_ref[n, 0] = kept[0]
        sums_ref[n, 1] = kept[1]
    for i in F_FORE:
        sent["fore"].append(wide.pull(get_f(i, 1), FV[i], rim_of_f))
    for i in F_BACK:
        sent["back"].append(wide.pull(get_f(i, 0), FV[i], rim_of_f))
    swap = odd("gx")
    packed = []
    for way in ("fore", "back"):
        fields = sent[way] + [functools.reduce(add, part[way])]
        rims = jnp.zeros((16, 128), F32)
        for j, field in enumerate(fields):
            if field[1] is not None:
                rims = jnp.where(lane // 8 == j, yroll(field[1], 8 * j + 4), rims)
        packed.append([field[0] for field in fields] + [rims])
    for j in range(SENT + 1):
        a_ref[j] = jnp.where(swap, packed[1][j], packed[0][j])
        b_ref[j] = jnp.where(swap, packed[0][j], packed[1][j])


def stream_rest(get_f, fs_ref):
    wide = Wide(lanes())
    for i, v in enumerate(FV):
        for r in range(2):
            if 0 <= r + v[0] < 2:
                put(fs_ref, i, r + v[0], wide.pull(get_f(i, r), v, fs_ref.shape[2] == 2))


def collide(hs_ref, fs_ref, sums_ref, a_ref, b_ref, solid_of, new_h, new_f, scratch, tiles, row_done=None):
    got_ref, phi_ref, grad_ref = scratch
    lane = lanes()
    wide = Wide(lane)
    swap = odd("gx")
    a, b = partner(a_ref, SENT, swap, True), partner(b_ref, SENT, swap, False)
    rims = jnp.where(swap, a, b), jnp.where(swap, b, a)
    for j in range(SENT):
        a, b = partner(a_ref, j, swap, True), partner(b_ref, j, swap, False)
        got_ref[0, j, 0] = jnp.where(swap, a, b)
        got_ref[1, j, 0] = jnp.where(swap, b, a)
        for n in range(2):
            got_ref[n, j, 1] = yroll(rims[n], -(8 * j + 4))

    def h_at(i, r, t, zs):
        if r == 0 and HV[i][0] == 1:
            return got_ref[0, H_FORE.index(i), t, zs]
        if r == 1 and HV[i][0] == -1:
            return got_ref[1, H_BACK.index(i), t, zs]
        return hs_ref[i, r, t, zs]

    def f_at(i, r, t, zs):
        if r == 0 and FV[i][0] == 1:
            return got_ref[0, len(H_FORE) + F_FORE.index(i), t, zs]
        if r == 1 and FV[i][0] == -1:
            return got_ref[1, len(H_BACK) + F_BACK.index(i), t, zs]
        return fs_ref[i, r, t, zs]

    every = slice(None)
    for t in range(2):
        phi_ref[0, t] = got_ref[0, SENT - 1, t] + sums_ref[1, t]
        phi_ref[3, t] = got_ref[1, SENT - 1, t] + sums_ref[0, t]
        for r in range(2):
            phi_ref[r + 1, t] = total(h_at(i, r, t, every) for i in range(NH))
    for r in range(2):
        below, own, above = [(phi_ref[q, 0], phi_ref[q, 1]) for q in (r, r + 1, r + 2)]
        across = (above[0] - below[0], above[1] - below[1])
        around = add(above, below)
        upright = tuple(zroll(own[t], 1) + zroll(own[t], -1) for t in range(2))
        third = tuple(
            (1.0 / 3.0) * own[t] + (1.0 / 6.0) * (around[t] + upright[t]) for t in range(2)
        )
        rim = tiles == 2
        third_up, third_down = wide.shift(third, -1, rim), wide.shift(third, 1, rim)
        across_up, across_down = wide.shift(across, -1, rim), wide.shift(across, 1, rim)
        own_up, own_down = wide.shift(own, -1, rim), wide.shift(own, 1, rim)
        for t in range(tiles):
            along_y = own_up[t] + own_down[t]
            level = (1.0 / 6.0) * own[t] + (1.0 / 12.0) * (around[t] + along_y)
            grad_ref[r, t, 0] = (1.0 / 6.0) * across[t] + (1.0 / 12.0) * (
                across_up[t] + across_down[t] + zroll(across[t], 1) + zroll(across[t], -1)
            )
            grad_ref[r, t, 1] = 0.5 * (third_up[t] - third_down[t])
            grad_ref[r, t, 2] = zroll(level, -1) - zroll(level, 1)
            grad_ref[r, t, 3] = (
                (1.0 / 3.0) * (around[t] + upright[t])
                + (1.0 / 6.0) * (zroll(around[t], 1) + zroll(around[t], -1))
                + (third_up[t] + third_down[t])
                - 4.0 * own[t]
            )
    for r in range(2):
        for t in range(tiles):
            for z in (0, 8):
                zs = slice(z, z + 8)
                solid = solid_of(r, t, zs)
                phi = phi_ref[r + 1, t, zs]
                grad = [grad_ref[r, t, n, zs] for n in range(3)]
                collide_part(
                    phi,
                    grad,
                    grad_ref[r, t, 3, zs],
                    solid,
                    lambda i, r=r, t=t, zs=zs: h_at(i, r, t, zs),
                    lambda i, r=r, t=t, zs=zs: f_at(i, r, t, zs),
                    functools.partial(new_h, r, t, zs),
                    functools.partial(new_f, r, t, zs),
                )
        if row_done is not None:
            row_done(r)


def dot(v, u):
    terms = [(s, c) for s, c in zip(v, u, strict=True) if s]
    out = None
    for s, c in terms:
        if out is None:
            out = c if s > 0 else -c
        else:
            out = out + c if s > 0 else out - c
    return out


def collide_part(phi, grad, laplacian, solid, h_at, f_at, put_h, put_f):
    clipped = jnp.clip(phi, 0.0, 1.0)
    density = 1.0 + 2.0 * clipped
    relax = 0.6 + 0.4 * clipped
    inverse = 1.0 / (density * relax)
    rate, per_density = density * inverse, relax * inverse
    potential = (4.0 * BETA) * phi * (phi - 1.0) * (phi - 0.5) - KAPPA * laplacian
    force = [potential * g for g in grad]
    squared = grad[0] * grad[0] + grad[1] * grad[1] + grad[2] * grad[2]
    scale = 1.0 / jnp.maximum(jnp.sqrt(squared), FLOOR)
    f_rest = f_at(0)
    moment = [0.5 * c for c in force]
    pressure = f_rest
    for i, o in FP:
        fi, fo = f_at(i), f_at(o)
        difference = fi - fo
        pressure = pressure + (fi + fo)
        for n in range(3):
            if FV[i][n]:
                moment[n] = (
                    moment[n] + difference if FV[i][n] > 0 else moment[n] - difference
                )
    u = [m * per_density for m in moment]
    speed = u[0] * u[0] + u[1] * u[1] + u[2] * u[2]
    pull = 3.0 * (1.0 - 0.5 * rate) * per_density
    drive = [3.0 * rate * u[n] + pull * force[n] for n in range(3)]
    keep = 1.0 - rate
    level = rate * (pressure - 1.5 * speed)
    bend = 4.5 * rate
    put_f(0, jnp.where(solid, f_rest, keep * f_rest + FW[0] * level))
    for i, o in FP:
        w = FW[i]
        fi, fo = f_at(i), f_at(o)
        along = dot(FV[i], u)
        even = w * (level + bend * (along * along))
        uneven = w * dot(FV[i], drive)
        put_f(i, jnp.where(solid, fo, keep * fi + (even + uneven)))
        put_f(o, jnp.where(solid, fi, keep * fo + (even - uneven)))
    sharp = LAMBDA * phi * (1.0 - phi) * scale
    drift = [3.0 * phi * u[n] + sharp * grad[n] for n in range(3)]
    h_rest = h_at(0)
    stay = 1.0 - INV_RELAX
    put_h(0, jnp.where(solid, h_rest, stay * h_rest + (INV_RELAX * HW[0]) * phi))
    for i, o in HP:
        w = INV_RELAX * HW[i]
        hi, ho = h_at(i), h_at(o)
        even = w * phi
        uneven = w * dot(HV[i], drift)
        put_h(i, jnp.where(solid, ho, stay * hi + (even + uneven)))
        put_h(o, jnp.where(solid, hi, stay * ho + (even - uneven)))


def first_kernel(h_ref, f_ref, s_ref, ya_ref, yb_ref, a_ref, b_ref, hs_ref, sums_ref, so_ref):
    rim = spread_edges(ya_ref, yb_ref)
    for r in range(2):
        so_ref[r, 0] = (s_ref[r] > 0).astype(F32)
        so_ref[r, 1] = rim("s", 0, r)
    stream(
        lambda i, r: (h_ref[i, r], rim("h", i, r)),
        lambda i, r: (f_ref[i, r], rim("f", i, r)),
        hs_ref,
        sums_ref,
        a_ref,
        b_ref,
        True,
    )


def first_rest_kernel(f_ref, ya_ref, yb_ref, fs_ref):
    rim = spread_edges(ya_ref, yb_ref)
    stream_rest(lambda i, r: (f_ref[i, r], rim("f", i, r)), fs_ref)


def middle_kernel(
    hs_ref, fs_ref, sums_ref, s_ref, ra_ref, rb_ref,
    a_ref, b_ref, hs2_ref, sums2_ref, f1_ref,
    h1_ref, got_ref, phi_ref, grad_ref,
):
    def new_h(r, t, zs, i, value):
        h1_ref[i, r, t, zs] = value

    def new_f(r, t, zs, i, value):
        f1_ref[i, r, t, zs] = value

    collide(
        hs_ref,
        fs_ref,
        sums_ref,
        ra_ref,
        rb_ref,
        lambda r, t, zs: s_ref[r, t, zs] > 0.5,
        new_h,
        new_f,
        (got_ref, phi_ref, grad_ref),
        2,
    )
    stream(
        lambda i, r: (h1_ref[i, r, 0], h1_ref[i, r, 1]),
        lambda i, r: (f1_ref[i, r, 0], f1_ref[i, r, 1]),
        hs2_ref,
        sums2_ref,
        a_ref,
        b_ref,
        False,
    )


def last_kernel(
    hs_ref, f1_ref, sums_ref, s_ref, ra_ref, rb_ref,
    h_hbm, f_hbm,
    h_ref, f_ref, fs_ref, got_ref, phi_ref, grad_ref, sems,
):
    stream_rest(lambda i, r: (f1_ref[i, r, 0], f1_ref[i, r, 1]), fs_ref)

    def new_h(r, t, zs, i, value):
        h_ref[r, i, zs] = value

    def new_f(r, t, zs, i, value):
        f_ref[r, i, zs] = value

    copies = []

    def row_done(r):
        for n, (source, target) in enumerate(((h_ref, h_hbm), (f_ref, f_hbm))):
            copies.append(
                pltpu.make_async_copy(source.at[r], target.at[:, r], sems.at[r, n])
            )
            copies[-1].start()

    collide(
        hs_ref,
        fs_ref,
        sums_ref,
        ra_ref,
        rb_ref,
        lambda r, t, zs: s_ref[r, t, zs] > 0.5,
        new_h,
        new_f,
        (got_ref, phi_ref, grad_ref),
        1,
        row_done,
    )
    for copy in copies:
        copy.wait()


HBM = pl.BlockSpec(memory_space=pltpu.HBM)
VMEM = pl.BlockSpec(memory_space=pltpu.VMEM)
TILE = (16, 128)
COVER = pl.CostEstimate(flops=2_000_000_000, bytes_accessed=4_000_000, transcendentals=0)
LIMIT = 16 * 1024 * 1024
NEAR_Y, FAR_Y, NEAR_X, FAR_X = True, False, True, False


def call(kernel, outs, *args, scratch=(), sems=None, source=VMEM, target=VMEM, cost=None):
    kept = [pltpu.VMEM(shape, F32) for shape in scratch]
    if sems is not None:
        kept.append(pltpu.SemaphoreType.DMA(sems))
    return pl.pallas_call(
        kernel,
        out_shape=[
            out if hasattr(out, "dtype") else jax.ShapeDtypeStruct(out, F32)
            for out in outs
        ],
        in_specs=[source] * len(args),
        out_specs=[target] * len(outs),
        scratch_shapes=kept,
        compiler_params=pltpu.CompilerParams(vmem_limit_bytes=LIMIT),
        cost_estimate=cost,
    )(*args)


def swap_near(block, axis, gather):
    n = lax.axis_size(axis)
    if gather:
        groups = [[i, i + 1] for i in range(0, n, 2)]
        return lax.all_gather(block, axis, axis_index_groups=groups)
    return lax.ppermute(block, axis, [(i, i ^ 1) for i in range(n)])


def swap_far(block, axis, gather):
    n = lax.axis_size(axis)
    if gather:
        groups = [[i, (i + 1) % n] for i in range(1, n, 2)]
        return lax.all_gather(block, axis, axis_index_groups=groups)
    route = [(i, (i + 1) % n if i % 2 else (i - 1) % n) for i in range(n)]
    return lax.ppermute(block, axis, route)


def shards(phase_pops, flow_pops, solid_flags):
    edge, sent = (EDGE_TILES, *TILE), (SENT + 1, *TILE)
    wide_h, wide_f = (NH, 2, 2, *TILE), (NF, 2, 2, *TILE)
    sums = (2, 2, *TILE)
    scratch = [(2, SENT, 2, *TILE), (4, 2, *TILE), (2, 2, 4, *TILE)]
    h, f = phase_pops, flow_pops
    (slot,) = call(slots_kernel, [jax.ShapeDtypeStruct(TILE, jnp.int32)], cost=COVER)
    a, b = call(edges_kernel, [edge, edge], slot, h, f, solid_flags)
    ya, yb = swap_near(a, "gy", NEAR_Y), swap_far(b, "gy", FAR_Y)
    a, b, hs, kept, solid = call(
        first_kernel, [sent, sent, wide_h, sums, (2, 2, *TILE)], h, f, solid_flags, ya, yb
    )
    a, b = swap_near(a, "gx", NEAR_X), swap_far(b, "gx", FAR_X)
    (fs,) = call(first_rest_kernel, [wide_f], f, ya, yb)
    a, b, hs, kept, f = call(
        middle_kernel,
        [sent, sent, wide_h, sums, wide_f],
        *(hs, fs, kept, solid, a, b),
        scratch=[wide_h, *scratch],
    )
    a, b = swap_near(a, "gx", NEAR_X), swap_far(b, "gx", FAR_X)
    out_h, out_f = (NH, 2, *TILE), (NF, 2, *TILE)
    return tuple(
        call(
            last_kernel,
            [out_h, out_f],
            *(hs, f, kept, solid, a, b),
            scratch=[(2, NH, *TILE), (2, NF, *TILE), (NF, 2, 1, *TILE), *scratch],
            sems=(2, 2),
            target=HBM,
        )
    )


def solution(mesh):
    placed = (P(None, "gx", None, "gy"), P(None, "gx", None, "gy"), P("gx", None, "gy"))
    return jax.shard_map(
        shards,
        mesh=mesh,
        in_specs=placed,
        out_specs=placed[:2],
        check_vma=False,
    )
```
